512 devices in a mesh: cfg: 2 (over y), space: 128 (over x, z), tm: 2 (over core).
Axes of the slice: x: 4, y: 2, z: 32, core: 2. Of those that a mesh axis runs over, the one named last changes fastest.
The devices are a block of a 4x8x32 slice.
Arguments:
- eigvecs: bfloat16 [4, 36864, 3, 2, 128], P(('cfg', 'tm'), 'space'), parts along dimension 0, may hold values from -24 to 24
- perambulator: bfloat16 [4, 8, 4, 2, 128, 128], P(('cfg', 'tm'), None, None, None, 'space'), parts along dimension 0, may hold values from -1 to 4
- momenta: int32 [1, 3], replicated, may hold values from 1 to 3
- source_slots: int32 [2], replicated, may hold values from 0 to 7, as said below
- gamma_columns: int32 [12, 4], replicated, may hold values from 0 to 3, each once within a row
- gamma_phases: int32 [12, 4], replicated, may hold values from 0 to 3
Outputs:
- meson: float32 [4, 128, 1, 12, 2, 128], P(('cfg', 'tm'), 'space'), parts along dimension 0
The draws below stay inside these ranges and needn't reach their ends.
There are 2 independent parts, one for each index of `cfg`. The reference program is written for one: setup_inputs(seed, part) draws one part's arguments, and reference() takes and returns one part's arrays. A program takes and returns all parts, laid end to end along the dimension named above; an argument that names none is the same for every part. Nothing has to cross between parts.
Inputs may be any that keep to these rules, and one draw needn't show every extreme that they name: `source_slots`: the two slots differ, and one of them is 7. `gamma_columns`: each row is a permutation of 0 to 3.
All inputs are finite; a program needn't handle non-finite values.
Results may differ from the reference program's by a relative error of at most 0.0049.
Values may be sent and summed in bfloat16 or wider, within the bound.
A program may use at most 64 MiB of HBM per device.

```python
import math
import jax
import jax.numpy as jnp
from jax import lax

NEV = 128
NSTORE = 8
NMOM = 1
NGAM = 12
LY = 48
LZ = 48
NT = 2
SITES = 36864
LX = 16


def draw_perambulator(key, part):
    noise_key = jax.random.fold_in(key, 11)
    diag_key = jax.random.fold_in(key, 23)
    shape = (NT, NSTORE, 4, 2, NEV, NEV)
    noise = jax.random.normal(noise_key, shape, jnp.float32) * (0.6 / math.sqrt(NEV))
    diagonal = jnp.exp(jax.random.uniform(diag_key, (NT, NSTORE, 4, NEV), jnp.float32, -0.7, 0.7))
    identity = jnp.eye(NEV, dtype=jnp.float32)
    real_part = noise[:, :, :, 0] + diagonal[:, :, :, :, None] * identity
    return jnp.stack([real_part, noise[:, :, :, 1]], axis=3).astype(jnp.bfloat16)


def draw_source_slots(key, part):
    other_key = jax.random.fold_in(key, 31)
    order_key = jax.random.fold_in(key, 37)
    other = jax.random.randint(other_key, (), 0, NSTORE - 1, jnp.int32)
    last = jnp.full((), NSTORE - 1, jnp.int32)
    order = jax.random.randint(order_key, (), 0, 2, jnp.int32)
    first = jnp.where(order == 0, other, last)
    second = jnp.where(order == 0, last, other)
    return jnp.stack([first, second]).astype(jnp.int32)


def set_ends(result, own_key, low, high):
    longest = result.shape.index(max(result.shape))
    spots = []
    for shift in (0, 1):
        where = [jax.random.randint(jax.random.fold_in(own_key, axis), (), 0, length) for axis, length in enumerate(result.shape)]
        where[longest] = (where[longest] + shift) % result.shape[longest]
        spots.append(tuple(where))
    return result.at[spots[0]].set(low).at[spots[1]].set(high)


def with_spikes(entries, rng, source, target, blocks, factor):
    def block_of(dim):
        return (jnp.arange(entries.shape[dim]) // (entries.shape[dim] // blocks)).reshape((-1,) + (1,) * (entries.ndim - 1 - dim))

    near = jax.random.permutation(rng, blocks)[block_of(target)]
    other_side = (block_of(target) + blocks // 2) % blocks
    return jnp.where((block_of(source) == near) | (block_of(source) == other_side), factor * entries, entries)


def block_levels(own_key, dims, cuts, smallest, largest):
    def one(position, shards_of):
        draws = jax.random.uniform(jax.random.fold_in(jax.random.fold_in(own_key, 6), position), (shards_of,), jnp.float32, smallest / len(cuts), largest / len(cuts))
        return jnp.repeat(jnp.exp(draws), dims[position] // shards_of).reshape((-1,) + (1,) * (len(dims) - position - 1))

    level = one(*cuts[0])
    for cut in cuts[1:]:
        level = level * one(*cut)
    return level


def heavy_noise(key, shape, scale, reach, pieces, heavy, kind=jnp.bfloat16):
    drawn = scale * jax.random.normal(key, shape, jnp.float32)
    if pieces:
        drawn = drawn * block_levels(key, shape, pieces, -0.22, 0.18)
    return jnp.clip(with_spikes(drawn, jax.random.fold_in(key, 3), *heavy), -reach, reach).astype(kind)


def setup_inputs(seed: int = 0, part: int = 0) -> dict:
    key_of = jax.random.split(jax.random.key(seed), 7)
    part_keys = jax.random.split(jax.random.fold_in(key_of[6], part), 7)
    eigvecs = heavy_noise(part_keys[0], (NT, SITES, 3, 2, NEV), 1.0, 24.0, ((0, 2), (1, 128)), (1, 4, 128, 5.5))
    perambulator = draw_perambulator(jax.random.fold_in(jax.random.fold_in(key_of[6], part), 71), part)
    momenta = jax.random.randint(key_of[2], (NMOM, 3), 1, 4).astype(jnp.int32)
    source_slots = draw_source_slots(jax.random.fold_in(key_of[6], 71), part)
    gamma_columns = jax.vmap(lambda own: jax.random.permutation(own, 4))(jax.random.split(key_of[4], NGAM)).reshape((NGAM, 4)).astype(jnp.int32)
    gamma_phases = set_ends(jax.random.randint(key_of[5], (NGAM, 4), 0, 4), jax.random.fold_in(key_of[5], 1), 0, 3).astype(jnp.int32)
    return dict(eigvecs=eigvecs, perambulator=perambulator, momenta=momenta, source_slots=source_slots, gamma_columns=gamma_columns, gamma_phases=gamma_phases)


def gamma_mixer(gamma_columns, gamma_phases):
    spin_ids = jnp.arange(4, dtype=jnp.int32)
    matches = (gamma_columns[:, :, None] == spin_ids[None, None, :]).astype(jnp.float32)
    real_sign = (gamma_phases == 0).astype(jnp.float32) - (gamma_phases == 2).astype(jnp.float32)
    imag_sign = (gamma_phases == 1).astype(jnp.float32) - (gamma_phases == 3).astype(jnp.float32)
    real_part = matches * real_sign[:, :, None]
    imag_part = matches * imag_sign[:, :, None]
    first_row = jnp.stack([real_part, -imag_part], axis=-1)
    second_row = jnp.stack([imag_part, real_part], axis=-1)
    return jnp.stack([first_row, second_row], axis=1)

def apply_gammas(blocks, gamma_mix, factor):
    return factor * jnp.einsum('gostk,apstkb->apgob', gamma_mix, blocks, precision=lax.Precision.HIGHEST)

def phase_tables(momenta, site_ids, extent_x):
    coord_z = site_ids % LZ
    coord_y = site_ids // LZ % LY
    coord_x = site_ids // (LY * LZ)
    turns = (momenta[:, 0:1] * coord_x[None, :] % extent_x).astype(jnp.float32) / extent_x + (momenta[:, 1:2] * coord_y[None, :] % LY).astype(jnp.float32) / LY + (momenta[:, 2:3] * coord_z[None, :] % LZ).astype(jnp.float32) / LZ
    angles = 2.0 * math.pi * turns
    return (jnp.cos(angles), jnp.sin(angles))

def sink_vectors(vectors, picked):
    eig_count = picked.shape[-1]
    real_parts = []
    imag_parts = []
    for spin_index in range(4):
        real_tau = picked[spin_index, 0]
        imag_tau = picked[spin_index, 1]
        stacked = jnp.concatenate([jnp.concatenate([real_tau, imag_tau], axis=1), jnp.concatenate([-imag_tau, real_tau], axis=1)], axis=0)
        product = jnp.dot(vectors, stacked, preferred_element_type=jnp.float32).astype(jnp.bfloat16)
        real_parts.append(product[:, :eig_count])
        imag_parts.append(product[:, eig_count:])
    return (jnp.stack(real_parts, axis=1), jnp.stack(imag_parts, axis=1))

def twisted(right_real, right_imag, cosine, sine):
    moment_count, site_count = cosine.shape
    shaped_real = right_real.astype(jnp.float32).reshape(1, site_count, 3, 4, -1)
    shaped_imag = right_imag.astype(jnp.float32).reshape(1, site_count, 3, 4, -1)
    cosine_wide = cosine.reshape(moment_count, site_count, 1, 1, 1)
    sine_wide = sine.reshape(moment_count, site_count, 1, 1, 1)
    wave_real = (cosine_wide * shaped_real - sine_wide * shaped_imag).astype(jnp.bfloat16)
    wave_imag = (sine_wide * shaped_real + cosine_wide * shaped_imag).astype(jnp.bfloat16)
    return (wave_real.reshape(moment_count, site_count * 3, 4, -1), wave_imag.reshape(moment_count, site_count * 3, 4, -1))

def reference(eigvecs, perambulator, momenta, source_slots, gamma_columns, gamma_phases):
    factor = 1.0 / math.sqrt(12.0 * SITES)
    site_ids = jnp.arange(SITES, dtype=jnp.int32)
    cosine, sine = phase_tables(momenta, site_ids, LX)
    gamma_mix = gamma_mixer(gamma_columns, gamma_phases)
    chosen = jnp.take(perambulator, source_slots.astype(jnp.int32), axis=1)
    row_total = SITES * 3
    results = []
    for time_index in range(NT):
        vectors = eigvecs[time_index].reshape(row_total, 2 * NEV)
        left_real, left_imag = sink_vectors(vectors, chosen[time_index, 0])
        right_real, right_imag = sink_vectors(vectors, chosen[time_index, 1])
        wave_real, wave_imag = twisted(right_real, right_imag, cosine, sine)
        flat_left_real = left_real.reshape(row_total, 4 * NEV)
        flat_left_imag = left_imag.reshape(row_total, 4 * NEV)
        per_momentum = []
        for moment_index in range(NMOM):
            flat_wave_real = wave_real[moment_index].reshape(row_total, 4 * NEV)
            flat_wave_imag = wave_imag[moment_index].reshape(row_total, 4 * NEV)
            real_block = jnp.dot(flat_left_real.T, flat_wave_real, preferred_element_type=jnp.float32) + jnp.dot(flat_left_imag.T, flat_wave_imag, preferred_element_type=jnp.float32)
            imag_block = jnp.dot(flat_left_real.T, flat_wave_imag, preferred_element_type=jnp.float32) - jnp.dot(flat_left_imag.T, flat_wave_real, preferred_element_type=jnp.float32)
            both_parts = jnp.stack([real_block, imag_block], axis=0).reshape(2, 4, NEV, 4, NEV)
            per_momentum.append(both_parts.transpose(2, 1, 3, 0, 4))
        blocks = jnp.stack(per_momentum, axis=1)
        results.append(apply_gammas(blocks, gamma_mix, factor))
    return jnp.stack(results, axis=0)
```

```python
import math

import jax
import jax.numpy as jnp
from jax import lax
from jax.sharding import Mesh
from jax.sharding import PartitionSpec as P

LY = 48
LZ = 48
SPACE = ("space_0", "space_1")


def gamma_mixer(gamma_columns, gamma_phases):
    spin_ids = jnp.arange(4, dtype=jnp.int32)
    matches = (gamma_columns[:, :, None] == spin_ids[None, None, :]).astype(jnp.float32)
    real_sign = (gamma_phases == 0).astype(jnp.float32) - (gamma_phases == 2).astype(jnp.float32)
    imag_sign = (gamma_phases == 1).astype(jnp.float32) - (gamma_phases == 3).astype(jnp.float32)
    real_part = matches * real_sign[:, :, None]
    imag_part = matches * imag_sign[:, :, None]
    first_row = jnp.stack([real_part, -imag_part], axis=-1)
    second_row = jnp.stack([imag_part, real_part], axis=-1)
    return jnp.stack([first_row, second_row], axis=1)


def phase_tables(momenta, site_ids, extent_x):
    coord_z = site_ids % LZ
    coord_y = site_ids // LZ % LY
    coord_x = site_ids // (LY * LZ)
    turns = (
        (momenta[:, 0:1] * coord_x[None, :] % extent_x).astype(jnp.float32) / extent_x
        + (momenta[:, 1:2] * coord_y[None, :] % LY).astype(jnp.float32) / LY
        + (momenta[:, 2:3] * coord_z[None, :] % LZ).astype(jnp.float32) / LZ
    )
    angles = 2.0 * math.pi * turns
    return (jnp.cos(angles), jnp.sin(angles))


HI = lax.Precision.HIGHEST


def on_device(eigvecs, perambulator, momenta, source_slots, gamma_columns, gamma_phases):
    local_sites = eigvecs.shape[1]
    eig_count = eigvecs.shape[4]
    ranks = lax.axis_size(SPACE)
    me = lax.axis_index(SPACE)
    total_sites = local_sites * ranks
    extent_x = total_sites // (LY * LZ)
    factor = 1.0 / math.sqrt(12.0 * total_sites)
    site_ids = me * local_sites + jnp.arange(local_sites, dtype=jnp.int32)
    cosine, sine = phase_tables(momenta, site_ids, extent_x)
    gamma_mix = gamma_mixer(gamma_columns, gamma_phases)
    selected = jnp.take(perambulator, source_slots, axis=1)[0, :, :, :, 0]
    chosen = lax.all_gather(selected, SPACE)
    vectors = eigvecs[0]
    wide = vectors.astype(jnp.float32)
    cw, sw = (cosine[0][:, None, None], sine[0][:, None, None])
    wave_real = cw * wide[:, :, 0] - sw * wide[:, :, 1]
    wave_imag = sw * wide[:, :, 0] + cw * wide[:, :, 1]
    turned = jnp.stack(
        [
            jnp.concatenate([wave_real, wave_imag], axis=-1),
            jnp.concatenate([wave_imag, -wave_real], axis=-1),
        ],
        axis=2,
    ).astype(jnp.bfloat16)
    rows = local_sites * 6
    overlap = lax.dot_general(
        vectors.reshape(rows, eig_count),
        turned.reshape(rows, 2 * eig_count),
        (((0,), (0,)), ((), ())),
        preferred_element_type=jnp.float32,
    )
    overlap = lax.psum(overlap, SPACE)
    m_real, m_imag = (overlap[:, :eig_count], overlap[:, eig_count:])
    left = lax.dynamic_index_in_dim(chosen[:, 0], me, axis=3, keepdims=False).astype(jnp.float32)
    left_real, left_imag = (left[:, :, 0], left[:, :, 1])
    dot = lambda a, b: lax.dot_general(a, b, (((0,), (0,)), ((), ())), precision=HI)
    x_real = dot(left_real, m_real) + dot(left_imag, m_imag)
    x_imag = dot(left_real, m_imag) - dot(left_imag, m_real)
    right = chosen[:, 1].astype(jnp.float32)
    mul = lambda a, b: jnp.einsum("sl,ltb->stb", a, b, precision=HI)
    a_real = mul(x_real, right[:, :, 0]) - mul(x_imag, right[:, :, 1])
    a_imag = mul(x_real, right[:, :, 1]) + mul(x_imag, right[:, :, 0])
    blocks = jnp.stack([a_real, a_imag], axis=2)
    meson = factor * jnp.einsum("gostk,stkb->gob", gamma_mix, blocks, precision=HI)
    return meson[None, None, None]


def solution(mesh):
    split = Mesh(
        mesh.devices.reshape(mesh.shape["cfg"], 4, 32, mesh.shape["tm"]),
        ("cfg", "space_0", "space_1", "tm"),
    )
    placed = (
        P(("cfg", "tm"), SPACE, None, None, None),
        P(("cfg", "tm"), None, None, None, SPACE, None),
        P(),
        P(),
        P(),
        P(),
    )
    return jax.shard_map(
        on_device,
        mesh=split,
        in_specs=placed,
        out_specs=P(("cfg", "tm"), SPACE, None, None, None, None),
        check_vma=False,
    )
```

```python
import math

import jax
import jax.numpy as jnp
from jax import lax
from jax.experimental import pallas as pl
from jax.experimental.pallas import tpu as pltpu
from jax.sharding import Mesh
from jax.sharding import PartitionSpec as P

LY = 48
LZ = 48
NX = 4
NZ = 32
WIN = 8
SPACE = ("space_0", "space_1")
NEAR = (-4, 3, -3, 2, -2, 1, -1)
FAR = (16, 8, 24)
BF = jnp.bfloat16
F32 = jnp.float32
MESH = pl.DeviceIdType.MESH


def iota(shape, dim):
    return lax.broadcasted_iota(jnp.int32, shape, dim)


def mm(a, b, dims):
    return lax.dot_general(a, b, (dims, ((), ())), preferred_element_type=F32)


def part_turns(momentum, coord, extent):
    product = (momentum * coord).astype(F32)
    return product / extent - jnp.floor(product / extent)


def wave_overlap(eig, tab_c, tab_s, line_c, line_s, lines, rows):
    even = (iota((rows, 128), 0) & 1) == 0
    flip = jnp.where(even, -1.0, 1.0).astype(F32)
    total = None
    for line in range(lines):
        block = eig[pl.ds(line * rows, rows), :]
        wide = block.astype(F32)
        other = jnp.where(even, pltpu.roll(wide, rows - 1, 0), pltpu.roll(wide, 1, 0))
        ca = line_c[line : line + 1, :]
        sa = line_s[line : line + 1, :]
        cb = tab_c[...]
        sb = tab_s[...]
        c = ca * cb - sa * sb
        s = sa * cb + ca * sb
        first = (c * wide + (s * flip) * other).astype(BF)
        second = (s * wide - (c * flip) * other).astype(BF)
        turned = jnp.concatenate([first, second], axis=1)
        product = mm(turned, block, ((0,), (0,)))
        total = product if total is None else total + product
    return total


def split(value):
    high = value.astype(BF)
    return high, (value - high.astype(F32)).astype(BF)


def kernel(
    lines, rows, extent_x, factor,
    eig_hbm, per_hbm, momenta, slots, columns, phases,
    out,
    eig, per, tab_c, tab_s, line_c, line_s,
    mst, xr, s1, nr, f1, fr, mq,
    p0x, gst, p0g, p1g, p1f, ast, ost, orv,
    loc_sem, t1, t2,
    xs, xrs, ns, nrs, fs, frs, gs, grs, hs, hrs, p0s, p0rs, p1s, p1rs, os_, ors,
):
    x = lax.axis_index("space_0")
    z = lax.axis_index("space_1")

    def at(dx, dz):
        return {
            "space_0": lax.rem(x + (dx + NX), NX),
            "space_1": lax.rem(z + (dz + NZ), NZ),
        }

    def zof(d):
        return lax.rem(z + (d + NZ), NZ)

    def push(src, dst, send, recv, device):
        return pltpu.make_async_remote_copy(
            src_ref=src, dst_ref=dst, send_sem=send, recv_sem=recv,
            device_id=device, device_id_type=MESH,
        )

    load_eig = pltpu.make_async_copy(eig_hbm, eig, loc_sem.at[0])
    load_per = pltpu.make_async_copy(per_hbm, per, loc_sem.at[1])
    load_eig.start()
    load_per.start()

    barrier = pltpu.get_barrier_semaphore()
    for d in (-4, 4, -3, 3, -2, 2, -1, 1):
        pl.semaphore_signal(barrier, inc=1, device_id=at(0, d), device_id_type=MESH)
    for d in range(1, NX):
        pl.semaphore_signal(barrier, inc=1, device_id=at(d, 0), device_id_type=MESH)

    inner = iota((rows, 128), 0) // 6
    angle = (2.0 * math.pi) * part_turns(momenta[0, 2], inner, LZ)
    tab_c[...] = jnp.cos(angle)
    tab_s[...] = jnp.sin(angle)
    line_ids = (x * NZ + z) * lines + iota((8, 128), 0)
    turns = part_turns(momenta[0, 0], line_ids // LY, extent_x) + part_turns(
        momenta[0, 1], lax.rem(line_ids, LY), LY
    )
    angle = (2.0 * math.pi) * turns
    line_c[...] = jnp.cos(angle)
    line_s[...] = jnp.sin(angle)

    load_per.wait()
    p0x[x] = per[slots[0]]
    p1g[z] = per[slots[1]]
    load_eig.wait()
    total = wave_overlap(eig, tab_c, tab_s, line_c, line_s, lines, rows)
    total = total.reshape(2, NX, 4, 8, 128)
    mst[:, 0:4] = total[0]
    mst[:, 4:8] = total[1]

    pl.semaphore_wait(barrier, 11)
    for d in (-4, 4):
        pl.semaphore_signal(t1, inc=1, device_id=at(0, d), device_id_type=MESH)

    x_copies = []
    for k, d in enumerate((2, 1, 3)):
        copy = push(mst.at[lax.rem(x + d, NX)], xr.at[k], xs.at[k], xrs.at[k], at(d, 0))
        copy.start()
        x_copies.append(copy)
    p0_copies = []
    for k, d in enumerate((2, 1, 3)):
        copy = push(p0x.at[x], p0x.at[x], hs.at[k], hrs.at[k], at(d, 0))
        copy.start()
        p0_copies.append(copy)
    pl.semaphore_wait(t1, 2)
    for d in (-8, 8):
        pl.semaphore_signal(t2, inc=1, device_id=at(0, d), device_id_type=MESH)
    for copy in x_copies:
        copy.wait_recv()
    s1[...] = mst[x] + xr[0] + xr[1] + xr[2]

    n_copies = []
    for k, d in enumerate(NEAR):
        copy = push(
            s1.at[lax.rem(z + (d + NZ), WIN)], nr.at[k], ns.at[k], nrs.at[k], at(0, d)
        )
        copy.start()
        n_copies.append(copy)

    for copy in p0_copies:
        copy.wait_recv()
    row = iota((128, 32), 0)
    source = (row >> 5) * 8 + ((row >> 2) & 3) * 2 + ((row >> 4) & 1)
    spread = jnp.where(iota((128, 32), 1) == source, 1.0, 0.0).astype(BF)
    tiles = p0x[...].astype(F32).reshape(32, 128).astype(BF)
    spread = mm(spread, tiles, ((1,), (0,)))
    mine = (iota((128, 128), 1) >> 5) == (iota((128, 128), 0) & 3)
    spread = jnp.where(mine, spread, 0.0).astype(BF)
    comb = jnp.where((iota((32, 128), 1) & 31) == iota((32, 128), 0), 1.0, 0.0).astype(BF)
    gst[...] = mm(comb, spread, ((1,), (1,))).reshape(32, 1, 128)
    p0g[z] = gst[z]

    for copy in n_copies:
        copy.wait_recv()
    value = s1[lax.rem(z, WIN)]
    for k in range(len(NEAR)):
        value = value + nr[k]
    f1[...] = value

    pl.semaphore_wait(t2, 2)
    f_copies = []
    for k, d in enumerate(FAR):
        copy = push(f1, fr.at[k], fs.at[k], frs.at[k], at(0, d))
        copy.start()
        f_copies.append(copy)

    def distance(i):
        half = i // 2
        return 16 + lax.rem(i, 2) * (2 * half + 1) - half

    def far_rows(i):
        d = distance(i)
        target = lax.rem(z + d, NZ)
        return (
            push(gst.at[target], p0g.at[z], p0s.at[i], p0rs.at[i], at(0, d)),
            push(p1g.at[z], p1g.at[z], p1s.at[i], p1rs.at[i], at(0, d)),
        )

    def far_start(i, carry):
        for copy in far_rows(i):
            copy.start()
        return carry

    def far_landed(i, carry):
        d = distance(i)
        src = lax.rem(z + (NZ - d), NZ)
        push(gst.at[src], p0g.at[src], p0s.at[i], p0rs.at[i], at(0, d)).wait_recv()
        push(p1g.at[src], p1g.at[src], p1s.at[i], p1rs.at[i], at(0, d)).wait_recv()
        return carry

    def far_sent(i, carry):
        for copy in far_rows(i):
            copy.wait_send()
        return carry

    lax.fori_loop(0, NZ - 1, far_start, 0)

    for copy in f_copies:
        copy.wait_recv()
    chunk = lax.rem(z, WIN)
    mq[chunk] = f1[...] + fr[0] + fr[1] + fr[2]
    g_copies = []
    for k, d in enumerate(NEAR):
        copy = push(mq.at[chunk], mq.at[chunk], gs.at[k], grs.at[k], at(0, d))
        copy.start()
        g_copies.append(copy)

    lax.fori_loop(0, NZ - 1, far_landed, 0)
    gathered = mm(p0g[...].reshape(32, 128).astype(BF), comb, ((0,), (0,)))
    mine = (iota((128, 128), 1) >> 5) == (iota((128, 128), 0) >> 5)
    left = jnp.where(mine, gathered, 0.0).reshape(4, 32, 128).sum(axis=0).astype(BF)
    p1f[...] = p1g[...].astype(F32).reshape(NZ * 8, 128)

    for k, d in enumerate(NEAR):
        src = lax.rem(z + (NZ - d), WIN)
        push(mq.at[src], mq.at[src], gs.at[k], grs.at[k], at(0, d)).wait_recv()
    halves = []
    for part in (0, 1):
        high, low = split(mq[4 * part : 4 * part + 4].reshape(32, 128))
        halves.append(mm(left, high, ((1,), (1,))) + mm(left, low, ((1,), (1,))))
    with_real, with_imag = halves
    x_real = with_real[0:16] + with_imag[16:32]
    x_imag = with_imag[0:16] - with_real[16:32]
    high, low = split(jnp.concatenate([x_real, x_imag], axis=0))
    stacked = jnp.concatenate([high, low], axis=0)
    for spin in range(4):
        made = []
        for part in (0, 1):
            right = p1f[pl.ds(2 * spin + part, NZ, stride=8), :].astype(BF)
            full = mm(stacked, right, ((1,), (0,)))
            made.append(full[0:32] + full[32:64])
        ast[spin, 0] = made[0][0:16] - made[1][16:32]
        ast[spin, 1] = made[1][0:16] + made[0][16:32]

    for gamma in range(columns.shape[0]):
        real = imag = None
        for spin in range(4):
            col = columns[gamma, spin]
            power = phases[gamma, spin]
            cr = jnp.where(power == 0, factor, 0.0) - jnp.where(power == 2, factor, 0.0)
            ci = jnp.where(power == 1, factor, 0.0) - jnp.where(power == 3, factor, 0.0)
            a_real = ast[col, 0, 4 * spin : 4 * spin + 4, :]
            a_imag = ast[col, 1, 4 * spin : 4 * spin + 4, :]
            part_r = cr * a_real - ci * a_imag
            part_i = cr * a_imag + ci * a_real
            real = part_r if real is None else real + part_r
            imag = part_i if imag is None else imag + part_i
        for k in range(NX):
            ost[k, 2 * gamma : 2 * gamma + 1, :] = real[k : k + 1]
            ost[k, 2 * gamma + 1 : 2 * gamma + 2, :] = imag[k : k + 1]

    o_copies = []
    for k, d in enumerate((2, 1, 3)):
        copy = push(ost.at[lax.rem(x + d, NX)], orv.at[k], os_.at[k], ors.at[k], at(d, 0))
        copy.start()
        o_copies.append(copy)
    for copy in o_copies:
        copy.wait_recv()
    out[...] = ost[x] + orv[0] + orv[1] + orv[2]

    lax.fori_loop(0, NZ - 1, far_sent, 0)
    for copy in x_copies + p0_copies + n_copies + f_copies + g_copies + o_copies:
        copy.wait_send()


def on_device(eigvecs, perambulator, momenta, source_slots, gamma_columns, gamma_phases):
    local_sites = eigvecs.shape[1]
    eig_count = eigvecs.shape[4]
    store_count = perambulator.shape[1]
    total_sites = local_sites * lax.axis_size(SPACE)
    extent_x = total_sites // (LY * LZ)
    lines = local_sites // LZ
    rows = LZ * 6
    assert local_sites == lines * LZ and eig_count == NX * NZ == 128 and lines <= 8
    count = gamma_columns.shape[0]
    vmem = lambda shape, dtype=F32: pltpu.VMEM(shape, dtype)
    dma = lambda n: pltpu.SemaphoreType.DMA((n,))
    import functools

    meson = pl.pallas_call(
        functools.partial(
            kernel, lines, rows, extent_x, 1.0 / math.sqrt(12.0 * total_sites)
        ),
        out_shape=jax.ShapeDtypeStruct((2 * count, 128), F32),
        in_specs=[pl.BlockSpec(memory_space=pl.ANY)] * 2
        + [pl.BlockSpec(memory_space=pltpu.SMEM)] * 4,
        out_specs=pl.BlockSpec(memory_space=pltpu.VMEM),
        scratch_shapes=[
            vmem((lines * rows, 128), BF),
            vmem((store_count, 8, 128), BF),
            vmem((rows, 128)),
            vmem((rows, 128)),
            vmem((8, 128)),
            vmem((8, 128)),
            vmem((NX, 8, 8, 128)),
            vmem((3, 8, 8, 128)),
            vmem((8, 8, 128)),
            vmem((7, 8, 128)),
            vmem((8, 128)),
            vmem((3, 8, 128)),
            vmem((8, 8, 128)),
            vmem((NX, 8, 128), BF),
            vmem((NZ, 1, 128)),
            vmem((NZ, 1, 128)),
            vmem((NZ, 8, 128), BF),
            vmem((NZ * 8, 128)),
            vmem((4, 2, 16, 128)),
            vmem((NX, 2 * count, 128)),
            vmem((3, 2 * count, 128)),
            dma(2),
            pltpu.SemaphoreType.REGULAR,
            pltpu.SemaphoreType.REGULAR,
            dma(3), dma(3), dma(7), dma(7), dma(3), dma(3), dma(7), dma(7),
            dma(3), dma(3), dma(31), dma(31), dma(31), dma(31), dma(3), dma(3),
        ],
        compiler_params=pltpu.CompilerParams(
            collective_id=0, has_side_effects=True, vmem_limit_bytes=24 * 1024 * 1024
        ),
        name="meson",
    )(
        eigvecs.reshape(local_sites * 6, eig_count),
        perambulator.reshape(store_count, 8, eig_count),
        momenta,
        source_slots,
        gamma_columns,
        gamma_phases,
    )
    return meson.reshape(1, 1, 1, count, 2, eig_count)


def solution(mesh):
    split_mesh = Mesh(
        mesh.devices.reshape(mesh.shape["cfg"], NX, NZ, mesh.shape["tm"]),
        ("cfg", "space_0", "space_1", "tm"),
    )
    placed = (
        P(("cfg", "tm"), SPACE, None, None, None),
        P(("cfg", "tm"), None, None, None, SPACE, None),
        P(),
        P(),
        P(),
        P(),
    )
    return jax.shard_map(
        on_device,
        mesh=split_mesh,
        in_specs=placed,
        out_specs=P(("cfg", "tm"), SPACE, None, None, None, None),
        check_vma=False,
    )
```

```python
import functools
import math

import jax
import jax.numpy as jnp
from jax import lax
from jax.experimental import pallas as pl
from jax.experimental.pallas import tpu as pltpu
from jax.sharding import Mesh
from jax.sharding import PartitionSpec as P

LY = 48
LZ = 48
NX = 4
NZ = 32
HALF = 17
STEP = 4
ROOT_UP = (4, 1, 2, 3)
ROOT_DOWN = (28, 29, 30)
HUBS = ((4, 5, 9), (9, 10, 17), (21, 17, 21), (26, 22, 26))
SPACE = ("space_0", "space_1")
BF = jnp.bfloat16
F32 = jnp.float32
MESH = pl.DeviceIdType.MESH


def iota(shape, dim):
    return lax.broadcasted_iota(jnp.int32, shape, dim)


def mm(a, b, dims):
    return lax.dot_general(a, b, (dims, ((), ())), preferred_element_type=F32)


def part_turns(momentum, coord, extent):
    product = (momentum * coord).astype(F32)
    return product / extent - jnp.floor(product / extent)


def wave_overlap(eig, tab_c, tab_s, line_c, line_s, lines, rows):
    even = (iota((rows, 128), 0) & 1) == 0
    total = None
    for line in range(lines):
        block = eig[pl.ds(line * rows, rows), :]
        wide = block.astype(F32)
        other = jnp.where(even, pltpu.roll(wide, rows - 1, 0), -pltpu.roll(wide, 1, 0))
        ca = line_c[line : line + 1, :]
        sa = line_s[line : line + 1, :]
        cb = tab_c[...]
        sb = tab_s[...]
        c = ca * cb - sa * sb
        s = sa * cb + ca * sb
        first = (c * wide + s * other).astype(BF)
        second = (s * wide - c * other).astype(BF)
        turned = jnp.concatenate([first, second], axis=1)
        product = mm(block, turned, ((0,), (0,)))
        total = product if total is None else total + product
    return total


def split(value):
    high = value.astype(BF)
    return high, (value - high.astype(F32)).astype(BF)


def kernel(
    lines, rows, extent_x, factor, count,
    eig_hbm, per_hbm, momenta, slots, columns, phases,
    out,
    eig, per, tab_c, tab_s, line_c, line_s,
    mst, xr, s1, mr, tm, p0x, gst, p0g, p1g, p1f, lft, ast, ost, orv,
    loc_sem, ready, xs, xrs, hs, hrs, p0s, p0r, p1s, p1r, ms, mrs, tr, os_, ors, o0s,
):
    x = lax.axis_index("space_0")
    z = lax.axis_index("space_1")
    w = lax.rem(z + (NZ - 1), NZ)
    last = NZ - 1

    def zof(v):
        return lax.rem(v + 1, NZ)

    def along_x(d):
        return {"space_0": lax.rem(x + d, NX), "space_1": z}

    def along_z(v):
        return {"space_0": x, "space_1": zof(v)}

    def push(src, dst, send, recv, device):
        return pltpu.make_async_remote_copy(
            src_ref=src, dst_ref=dst, send_sem=send, recv_sem=recv,
            device_id=device, device_id_type=MESH,
        )

    def loop(lower, upper, body):
        def step(v, carry):
            body(v)
            return carry

        lax.fori_loop(lower, upper, step, 0)

    load_eig = pltpu.make_async_copy(eig_hbm, eig, loc_sem.at[0])
    load_per = pltpu.make_async_copy(per_hbm, per, loc_sem.at[1])
    load_eig.start()
    load_per.start()

    barrier = pltpu.get_barrier_semaphore()
    for d in range(1, NX):
        pl.semaphore_signal(barrier, inc=1, device_id=along_x(d), device_id_type=MESH)

    def greet(v):
        pl.semaphore_signal(barrier, inc=1, device_id=along_z(v), device_id_type=MESH)

    loop(w + 1, NZ, greet)

    inner = iota((rows, 128), 0) // 6
    angle = (2.0 * math.pi) * part_turns(momenta[0, 2], inner, LZ)
    tab_c[...] = jnp.cos(angle)
    tab_s[...] = jnp.sin(angle)
    line_ids = (x * NZ + z) * lines + iota((8, 128), 0)
    turns = part_turns(momenta[0, 0], line_ids // LY, extent_x) + part_turns(
        momenta[0, 1], lax.rem(line_ids, LY), LY
    )
    angle = (2.0 * math.pi) * turns
    line_c[...] = jnp.cos(angle)
    line_s[...] = jnp.sin(angle)

    load_per.wait()
    p0x[x] = per[slots[0]]
    p1g[z] = per[slots[1]]
    load_eig.wait()
    total = wave_overlap(eig, tab_c, tab_s, line_c, line_s, lines, rows)
    mst[:, 0:4] = total[:, 0:128].reshape(NX, 4, 8, 128)
    mst[:, 4:8] = total[:, 128:256].reshape(NX, 4, 8, 128)

    pl.semaphore_wait(barrier, w + (NX - 1))

    for hub_w, first, stop in HUBS[2:]:

        @pl.when(w == hub_w)
        def _():
            def tell(v):
                pl.semaphore_signal(ready, inc=1, device_id=along_z(v), device_id_type=MESH)

            loop(first, stop, tell)

    p0_copies = []
    x_copies = []
    for k, d in enumerate((2, 1, 3)):
        copy = push(p0x.at[x], p0x.at[x], hs.at[k], hrs.at[k], along_x(d))
        copy.start()
        p0_copies.append(copy)
    for k, d in enumerate((2, 1, 3)):
        copy = push(mst.at[lax.rem(x + d, NX)], xr.at[k], xs.at[k], xrs.at[k], along_x(d))
        copy.start()
        x_copies.append(copy)

    def right_tile(v):
        return push(p1g.at[z], p1g.at[z], p1s.at[v], p1r.at[w], along_z(v))

    def left_row(v):
        return push(
            gst.at[pl.ds(zof(v), 1)], p0g.at[z, pl.ds(1, 1)], p0s.at[v], p0r.at[w], along_z(v)
        )

    def left_rows_root():
        return push(gst.at[pl.ds(0, 2)], p0g.at[z], p0s.at[0], p0r.at[w], along_z(0))

    loop(0, w, lambda v: right_tile(v).start())
    for copy in p0_copies:
        copy.wait_recv()
    row = iota((128, 32), 0)
    source = (row >> 5) * 8 + ((row >> 2) & 3) * 2 + ((row >> 4) & 1)
    spread = jnp.where(iota((128, 32), 1) == source, 1.0, 0.0).astype(BF)
    tiles = p0x[...].astype(F32).reshape(32, 128).astype(BF)
    spread = mm(spread, tiles, ((1,), (0,)))
    mine = (iota((128, 128), 1) >> 5) == (iota((128, 128), 0) & 3)
    spread = jnp.where(mine, spread, 0.0).astype(BF)
    comb = jnp.where((iota((32, 128), 1) & 31) == iota((32, 128), 0), 1.0, 0.0).astype(BF)
    gst[...] = mm(comb, spread, ((1,), (1,))).reshape(32, 1, 128)

    @pl.when(w > 0)
    def _():
        p0g[z, 1] = gst[z]
        left_rows_root().start()

    @pl.when(w == 0)
    def _():
        p0g[z] = gst[0:2]

    loop(1, w, lambda v: left_row(v).start())

    for copy in x_copies:
        copy.wait_recv()
    s1[...] = mst[x] + xr[0] + xr[1] + xr[2]

    def within(first, stop):
        return (w >= first) & (w < stop)

    parent = jnp.where(within(5, 9), 4, 0)
    parent = jnp.where(within(10, 17), 9, parent)
    parent = jnp.where(within(17, 21), 21, parent)
    parent = jnp.where(within(22, 26), 26, parent)

    def to_parent():
        return push(s1, mr.at[w], ms.at[NZ], mrs.at[w], along_z(parent))

    def summed(first, stop):
        def gather(v, value):
            push(s1, mr.at[v], ms.at[NZ], mrs.at[v], along_z(v)).wait_recv()
            return value + mr[v]

        s1[...] = lax.fori_loop(first, stop, gather, s1[...])

    for first, stop in ((17, 21), (22, 26)):

        @pl.when(within(first, stop))
        def _():
            pl.semaphore_wait(ready, 1)

    for hub_w, first, stop in HUBS:

        @pl.when(w == hub_w)
        def _():
            summed(first, stop)

    @pl.when(w > 0)
    def _():
        to_parent().start()

    def answer(v):
        right_tile(v).start()
        left_row(v).start()

    def landed(v):
        src = zof(v)
        push(p1g.at[src], p1g.at[src], p1s.at[v], p1r.at[v], along_z(v)).wait_recv()
        push(
            gst.at[pl.ds(0, 1)], p0g.at[src, pl.ds(1, 1)], p0s.at[v], p0r.at[v], along_z(v)
        ).wait_recv()

    def landed_root(v):
        src = zof(v)
        push(p1g.at[src], p1g.at[src], p1s.at[v], p1r.at[v], along_z(v)).wait_recv()
        push(gst.at[pl.ds(0, 2)], p0g.at[src], p0s.at[v], p0r.at[v], along_z(v)).wait_recv()

    @pl.when(w == 0)
    def _():
        def meet(v):
            landed_root(v)
            answer(v)

        loop(1, last, meet)
        landed_root(last)

    @pl.when((w > 0) & (w < last))
    def _():
        def meet(v):
            landed(v)
            answer(v)

        loop(w + 1, last, meet)
        landed(last)
        loop(0, w, landed)

    def prepare(slot):
        rows_ = p0g[:, slot].reshape(32, 128).astype(BF)
        gathered = mm(rows_, comb, ((0,), (0,)))
        mine_ = (iota((128, 128), 1) >> 5) == (iota((128, 128), 0) >> 5)
        lft[slot] = jnp.where(mine_, gathered, 0.0).reshape(4, 32, 128).sum(axis=0).astype(BF)

    def project(slot):
        left = lft[slot]
        halves = []
        for part in (0, 1):
            high, low = split(tm[4 * part : 4 * part + 4].reshape(32, 128))
            halves.append(mm(left, high, ((1,), (1,))) + mm(left, low, ((1,), (1,))))
        with_real, with_imag = halves
        x_real = with_real[0:16] + with_imag[16:32]
        x_imag = with_imag[0:16] - with_real[16:32]
        high, low = split(jnp.concatenate([x_real, x_imag], axis=0))
        stacked = jnp.concatenate([high, low], axis=0)
        for spin in range(4):
            made = []
            for part in (0, 1):
                right = p1f[pl.ds(2 * spin + part, NZ, stride=8), :].astype(BF)
                full = mm(stacked, right, ((1,), (0,)))
                made.append(full[0:32] + full[32:64])
            ast[spin, 0] = made[0][0:16] - made[1][16:32]
            ast[spin, 1] = made[1][0:16] + made[0][16:32]
        for gamma in range(count):
            real = imag = None
            for spin in range(4):
                col = columns[spin, gamma]
                power = phases[spin, gamma]
                cr = jnp.where(power == 0, factor, 0.0) - jnp.where(power == 2, factor, 0.0)
                ci = jnp.where(power == 1, factor, 0.0) - jnp.where(power == 3, factor, 0.0)
                a_real = ast[col, 0, 4 * spin : 4 * spin + 4, :]
                a_imag = ast[col, 1, 4 * spin : 4 * spin + 4, :]
                part_r = cr * a_real - ci * a_imag
                part_i = cr * a_imag + ci * a_real
                real = part_r if real is None else real + part_r
                imag = part_i if imag is None else imag + part_i
            for k in range(NX):
                ost[slot, k, 2 * gamma : 2 * gamma + 1, :] = real[k : k + 1]
                ost[slot, k, 2 * gamma + 1 : 2 * gamma + 2, :] = imag[k : k + 1]

    def total_to(v):
        return push(tm, tm, ms.at[v], tr, along_z(v))

    upward = w < HALF
    hub = jnp.where(upward, lax.rem(w, STEP) == 0, lax.rem(NZ - w, STEP) == 0)
    near_first = jnp.where(upward, w + 1, jnp.maximum(w - STEP, HALF))
    near_stop = jnp.where(upward, jnp.minimum(w + STEP + 1, HALF), w)

    def relay(act):
        @pl.when(hub & (w > 0) & (w < last))
        def _():
            loop(0, near_stop - near_first, lambda i: act(jnp.where(upward, near_stop - 1 - i, near_first + i)))

    def relay_root(act):
        for v in ROOT_UP + ROOT_DOWN:
            act(v)

    def rows_to_last(k):
        return push(
            ost.at[0, k], orv.at[x], o0s.at[k], ors.at[x], {"space_0": k, "space_1": zof(last)}
        )

    def rows_to_x(d):
        k = lax.rem(x + d, NX)
        return push(ost.at[1, k], orv.at[x], os_.at[d - 1], ors.at[x], along_x(d))

    def rows_from(k):
        push(ost.at[1, k], orv.at[k], os_.at[0], ors.at[k], along_x(1)).wait_recv()

    @pl.when(w == 0)
    def _():
        prepare(0)
        prepare(1)
        p1f[...] = p1g[...].astype(F32).reshape(NZ * 8, 128)

        summed(1, 5)
        summed(9, 10)
        summed(21, 22)
        summed(26, NZ)
        tm[...] = s1[...]
        for v in ROOT_UP:
            total_to(v).start()
        project(0)
        for k in range(NX):
            rows_to_last(k).start()
        for v in ROOT_DOWN:
            total_to(v).start()

    @pl.when((w > 0) & (w < last))
    def _():
        prepare(1)
        p1f[...] = p1g[...].astype(F32).reshape(NZ * 8, 128)
        total_to(w).wait_recv()

    relay(lambda v: total_to(v).start())

    @pl.when(w < last)
    def _():
        project(1)
        for d in (2, 1, 3):
            rows_to_x(d).start()

    @pl.when(w < last)
    def _():
        for d in (1, 3, 2):
            rows_from(lax.rem(x + d, NX))
        orv[x] = ost[1, x]

    @pl.when(w == last)
    def _():
        for k in range(NX):
            rows_from(k)

    out[...] = orv[0] + orv[1] + orv[2] + orv[3]

    for copy in x_copies + p0_copies:
        copy.wait_send()

    @pl.when(w > 0)
    def _():
        to_parent().wait_send()
        left_rows_root().wait_send()

    loop(0, w, lambda v: right_tile(v).wait_send())
    loop(1, w, lambda v: left_row(v).wait_send())

    def answered(v):
        right_tile(v).wait_send()
        left_row(v).wait_send()

    loop(w + 1, last, answered)

    @pl.when(w == 0)
    def _():
        relay_root(lambda v: total_to(v).wait_send())
        for k in range(NX):
            rows_to_last(k).wait_send()

    relay(lambda v: total_to(v).wait_send())

    @pl.when(w < last)
    def _():
        for d in (2, 1, 3):
            rows_to_x(d).wait_send()


def on_device(eigvecs, perambulator, momenta, source_slots, gamma_columns, gamma_phases):
    local_sites = eigvecs.shape[1]
    eig_count = eigvecs.shape[4]
    store_count = perambulator.shape[1]
    total_sites = local_sites * lax.axis_size(SPACE)
    extent_x = total_sites // (LY * LZ)
    lines = local_sites // LZ
    rows = LZ * 6
    assert local_sites == lines * LZ and eig_count == NX * NZ == 128 and lines <= 8
    count = gamma_columns.shape[0]
    vmem = lambda shape, dtype=F32: pltpu.VMEM(shape, dtype)
    dma = lambda n: pltpu.SemaphoreType.DMA((n,))

    meson = pl.pallas_call(
        functools.partial(
            kernel, lines, rows, extent_x, 1.0 / math.sqrt(12.0 * total_sites), count
        ),
        out_shape=jax.ShapeDtypeStruct((2 * count, 128), F32),
        in_specs=[pl.BlockSpec(memory_space=pltpu.HBM)] * 2
        + [pl.BlockSpec(memory_space=pltpu.SMEM)] * 4,
        out_specs=pl.BlockSpec(memory_space=pltpu.VMEM),
        scratch_shapes=[
            vmem((lines * rows, 128), BF),
            vmem((store_count, 8, 128), BF),
            vmem((rows, 128)),
            vmem((rows, 128)),
            vmem((8, 128)),
            vmem((8, 128)),
            vmem((NX, 8, 8, 128)),
            vmem((3, 8, 8, 128)),
            vmem((8, 8, 128)),
            vmem((NZ, 8, 8, 128)),
            vmem((8, 8, 128)),
            vmem((NX, 8, 128), BF),
            vmem((NZ, 1, 128)),
            vmem((NZ, 2, 1, 128)),
            vmem((NZ, 8, 128), BF),
            vmem((NZ * 8, 128)),
            vmem((2, 32, 128), BF),
            vmem((4, 2, 16, 128)),
            vmem((2, NX, 2 * count, 128)),
            vmem((NX, 2 * count, 128)),
            dma(2),
            pltpu.SemaphoreType.REGULAR,
            dma(3), dma(3), dma(3), dma(3),
            dma(NZ), dma(NZ), dma(NZ), dma(NZ), dma(NZ + 1), dma(NZ),
            pltpu.SemaphoreType.DMA,
            dma(3), dma(NX), dma(NX),
        ],
        compiler_params=pltpu.CompilerParams(
            collective_id=0, has_side_effects=True, vmem_limit_bytes=67043328
        ),
        name="meson",
    )(
        eigvecs.reshape(local_sites * 6, eig_count),
        perambulator.reshape(store_count, 8, eig_count),
        momenta,
        source_slots,
        gamma_columns.T,
        gamma_phases.T,
    )
    return meson.reshape(1, 1, 1, count, 2, eig_count)


def solution(mesh):
    split_mesh = Mesh(
        mesh.devices.reshape(mesh.shape["cfg"], NX, NZ, mesh.shape["tm"]),
        ("cfg", "space_0", "space_1", "tm"),
    )
    placed = (
        P(("cfg", "tm"), SPACE, None, None, None),
        P(("cfg", "tm"), None, None, None, SPACE, None),
        P(),
        P(),
        P(),
        P(),
    )
    return jax.shard_map(
        on_device,
        mesh=split_mesh,
        in_specs=placed,
        out_specs=P(("cfg", "tm"), SPACE, None, None, None, None),
        check_vma=False,
    )
```

```python
import functools
import math

import jax
import jax.numpy as jnp
from jax import lax
from jax.experimental import pallas as pl
from jax.experimental.pallas import tpu as pltpu
from jax.sharding import Mesh
from jax.sharding import PartitionSpec as P

LY = 48
LZ = 48
NX = 4
NZ = 32
HALF = 17
STEP = 4
LAG = 6
HUBS = ((4, 5, 9), (9, 10, 14), (19, 17, 19), (22, 20, 22), (25, 23, 25), (28, 26, 28))
ROOT_UP = (4, 1, 2, 3)
ROOT_DOWN = (22, 28, 29, 30)
DOWN = ((28, 24, 28), (22, 17, 22), (22, 23, 24))
SPACE = ("space_0", "space_1")
BF = jnp.bfloat16
F32 = jnp.float32
WIRE = F32
MESH = pl.DeviceIdType.MESH


def iota(shape, dim):
    return lax.broadcasted_iota(jnp.int32, shape, dim)


def mm(a, b, dims):
    return lax.dot_general(a, b, (dims, ((), ())), preferred_element_type=F32)


def part_turns(momentum, coord, extent):
    product = (momentum * coord).astype(F32)
    return product / extent - jnp.floor(product / extent)


def wave_overlap(eig, tab_c, tab_s, line_c, line_s, lines, rows):
    even = (iota((rows, 128), 0) & 1) == 0
    total = None
    for line in range(lines):
        block = eig[pl.ds(line * rows, rows), :]
        wide = block.astype(F32)
        other = jnp.where(even, pltpu.roll(wide, rows - 1, 0), -pltpu.roll(wide, 1, 0))
        ca = line_c[line : line + 1, :]
        sa = line_s[line : line + 1, :]
        cb = tab_c[...]
        sb = tab_s[...]
        c = ca * cb - sa * sb
        s = sa * cb + ca * sb
        first = (c * wide + s * other).astype(BF)
        second = (s * wide - c * other).astype(BF)
        turned = jnp.concatenate([first, second], axis=1)
        product = mm(block, turned, ((0,), (0,)))
        total = product if total is None else total + product
    return total


def split(value):
    high = value.astype(BF)
    return high, (value - high.astype(F32)).astype(BF)


def kernel(
    lines, rows, extent_x, factor, count,
    eig_hbm, per_hbm, mom_hbm, slots_hbm, col_hbm, pha_hbm,
    out,
    momenta, slots, columns, phases,
    eig, per, tab_c, tab_s, line_c, line_s,
    mst, xr, s1, s1b, mr, tm, p0x, gst, p0g, p1g, p1f, lft, ast, ost, orv,
    loc_sem, ready, xs, xrs, hs, hrs, p0s, p0r, p1s, p1r, ms, mrs, tr, ls, lr, os_, ors, o0s,
):
    x = lax.axis_index("space_0")
    z = lax.axis_index("space_1")
    w = lax.rem(z + (NZ - 1), NZ)
    last = NZ - 1

    def zof(v):
        return lax.rem(v + 1, NZ)

    def along_x(d):
        return {"space_0": lax.rem(x + d, NX), "space_1": z}

    def along_z(v):
        return {"space_0": x, "space_1": zof(v)}

    def push(src, dst, send, recv, device):
        return pltpu.make_async_remote_copy(
            src_ref=src, dst_ref=dst, send_sem=send, recv_sem=recv,
            device_id=device, device_id_type=MESH,
        )

    def loop(lower, upper, body):
        def step(v, carry):
            body(v)
            return carry

        lax.fori_loop(lower, upper, step, 0)

    pairs = (
        (mom_hbm, momenta), (eig_hbm, eig), (slots_hbm, slots),
        (per_hbm, per), (col_hbm, columns), (pha_hbm, phases),
    )
    loads = [pltpu.make_async_copy(a, b, loc_sem.at[k]) for k, (a, b) in enumerate(pairs)]
    for load in loads:
        load.start()
    load_mom, load_eig, load_slots, load_per, load_col, load_pha = loads

    barrier = pltpu.get_barrier_semaphore()
    for d in range(1, NX):
        pl.semaphore_signal(barrier, inc=1, device_id=along_x(d), device_id_type=MESH)

    def greet(v):
        pl.semaphore_signal(barrier, inc=1, device_id=along_z(v), device_id_type=MESH)

    loop(w + 1, NZ, greet)

    load_mom.wait()
    inner = iota((rows, 128), 0) // 6
    angle = (2.0 * math.pi) * part_turns(momenta[0, 2], inner, LZ)
    tab_c[...] = jnp.cos(angle)
    tab_s[...] = jnp.sin(angle)
    line_ids = (x * NZ + z) * lines + iota((8, 128), 0)
    turns = part_turns(momenta[0, 0], line_ids // LY, extent_x) + part_turns(
        momenta[0, 1], lax.rem(line_ids, LY), LY
    )
    angle = (2.0 * math.pi) * turns
    line_c[...] = jnp.cos(angle)
    line_s[...] = jnp.sin(angle)

    load_slots.wait()
    load_per.wait()
    p0x[x] = per[slots[0]]
    p1g[w] = per[slots[1]]
    load_col.wait()
    load_pha.wait()
    pl.semaphore_wait(barrier, w + (NX - 1))

    for hub, first, stop in HUBS:
        if hub > first:

            @pl.when(w == hub)
            def _():
                def tell(v):
                    pl.semaphore_signal(ready, inc=1, device_id=along_z(v), device_id_type=MESH)

                loop(first, stop, tell)

    p0_copies = []
    for k, d in enumerate((2, 1, 3)):
        copy = push(p0x.at[x], p0x.at[x], hs.at[k], hrs.at[k], along_x(d))
        copy.start()
        p0_copies.append(copy)
    def right_tile(v):
        return push(p1g.at[w], p1g.at[w], p1s.at[v], p1r.at[w], along_z(v))

    def left_row(v):
        return push(
            gst.at[pl.ds(zof(v), 1)], p0g.at[z, pl.ds(1, 1)], p0s.at[v], p0r.at[w], along_z(v)
        )

    def left_rows_root():
        return push(gst.at[pl.ds(0, 2)], p0g.at[z], p0s.at[0], p0r.at[w], along_z(0))

    direct = jnp.where(w < HALF, 1, HALF)

    @pl.when(w > 0)
    def _():
        right_tile(0).start()

    load_eig.wait()
    total = wave_overlap(eig, tab_c, tab_s, line_c, line_s, lines, rows)
    mst[:, 0:32] = total[:, 0:128].reshape(NX, 32, 128)
    mst[:, 32:64] = total[:, 128:256].reshape(NX, 32, 128)
    x_copies = []
    for k, d in enumerate((2, 1, 3)):
        copy = push(mst.at[lax.rem(x + d, NX)], xr.at[k], xs.at[k], xrs.at[k], along_x(d))
        copy.start()
        x_copies.append(copy)
    loop(direct, w, lambda v: right_tile(v).start())
    for copy in p0_copies:
        copy.wait_recv()
    row = iota((128, 32), 0)
    source = (row >> 5) * 8 + ((row >> 2) & 3) * 2 + ((row >> 4) & 1)
    spread = jnp.where(iota((128, 32), 1) == source, 1.0, 0.0).astype(BF)
    tiles = p0x[...].astype(F32).reshape(32, 128).astype(BF)
    spread = mm(spread, tiles, ((1,), (0,)))
    mine = (iota((128, 128), 1) >> 5) == (iota((128, 128), 0) & 3)
    spread = jnp.where(mine, spread, 0.0).astype(BF)
    comb = jnp.where((iota((32, 128), 1) & 31) == iota((32, 128), 0), 1.0, 0.0).astype(BF)
    gst[...] = mm(comb, spread, ((1,), (1,))).reshape(32, 1, 128)

    @pl.when(w > 0)
    def _():
        p0g[z, 1] = gst[z]
        left_rows_root().start()

    @pl.when(w == 0)
    def _():
        p0g[z] = gst[0:2]

    loop(1, w, lambda v: left_row(v).start())

    for copy in x_copies:
        copy.wait_recv()
    value = mst[x] + xr[0] + xr[1] + xr[2]
    s1[...] = value

    def parent_of(v):
        parent = 0
        for hub, first, stop in HUBS:
            parent = jnp.where((v >= first) & (v < stop), hub, parent)
        return parent

    def to_parent():
        return push(s1b, mr.at[w], ms.at[NZ], mrs.at[w], along_z(parent_of(w)))

    def add(v):
        push(s1b, mr.at[v], ms.at[NZ], mrs.at[v], along_z(v)).wait_recv()
        s1[...] += mr[v].astype(F32)

    for hub, first, stop in HUBS:

        @pl.when(w == hub)
        def _():
            loop(first, stop, add)

        if hub > first:

            @pl.when((w >= first) & (w < stop))
            def _():
                pl.semaphore_wait(ready, 1)

    s1b[...] = s1[...].astype(WIRE)

    @pl.when(w > 0)
    def _():
        to_parent().start()

    def add_direct(v):
        @pl.when(parent_of(v) == 0)
        def _():
            add(v)

    def answer(v):
        right_tile(v).start()
        left_row(v).start()

    def landed_tile(v):
        push(p1g.at[v], p1g.at[v], p1s.at[v], p1r.at[v], along_z(v)).wait_recv()

    def landed(v):
        src = zof(v)

        @pl.when((v < HALF) | (w >= HALF))
        def _():
            landed_tile(v)

        push(
            gst.at[pl.ds(0, 1)], p0g.at[src, pl.ds(1, 1)], p0s.at[v], p0r.at[v], along_z(v)
        ).wait_recv()

    def landed_root(v):
        src = zof(v)
        landed_tile(v)
        push(gst.at[pl.ds(0, 2)], p0g.at[src], p0s.at[v], p0r.at[v], along_z(v)).wait_recv()

    @pl.when(w == 0)
    def _():
        def meet(v):
            landed_root(v)
            answer(v)

            @pl.when(v > LAG)
            def _():
                add_direct(v - LAG)

        loop(1, last, meet)
        landed_root(last)
        add_direct(last - LAG)

    @pl.when((w > 0) & (w < last))
    def _():
        def meet(v):
            landed(v)
            answer(v)

        loop(w + 1, last, meet)
        landed(last)
        loop(0, w, landed)

    def prepare(slot):
        rows_ = p0g[:, slot].reshape(32, 128).astype(BF)
        gathered = mm(rows_, comb, ((0,), (0,)))
        mine_ = (iota((128, 128), 1) >> 5) == (iota((128, 128), 0) >> 5)
        lft[slot] = jnp.where(mine_, gathered, 0.0).reshape(4, 32, 128).sum(axis=0).astype(BF)

    def project(slot):
        left = lft[slot]
        halves = []
        for part in (0, 1):
            high, low = split(tm[32 * part : 32 * part + 32])
            halves.append(mm(left, high, ((1,), (1,))) + mm(left, low, ((1,), (1,))))
        with_real, with_imag = halves
        x_real = with_real[0:16] + with_imag[16:32]
        x_imag = with_imag[0:16] - with_real[16:32]
        high, low = split(jnp.concatenate([x_real, x_imag], axis=0))
        stacked = jnp.concatenate([high, low], axis=0)
        for spin in range(4):
            made = []
            for part in (0, 1):
                right = p1f[pl.ds(2 * spin + part, NZ, stride=8), :].astype(BF)
                full = mm(stacked, right, ((1,), (0,)))
                made.append(full[0:32] + full[32:64])
            ast[spin, 0] = made[0][0:16] - made[1][16:32]
            ast[spin, 1] = made[1][0:16] + made[0][16:32]
        for gamma in range(count):
            real = imag = None
            for spin in range(4):
                col = columns[spin, gamma]
                power = phases[spin, gamma]
                cr = jnp.where(power == 0, factor, 0.0) - jnp.where(power == 2, factor, 0.0)
                ci = jnp.where(power == 1, factor, 0.0) - jnp.where(power == 3, factor, 0.0)
                a_real = ast[col, 0, 4 * spin : 4 * spin + 4, :]
                a_imag = ast[col, 1, 4 * spin : 4 * spin + 4, :]
                part_r = cr * a_real - ci * a_imag
                part_i = cr * a_imag + ci * a_real
                real = part_r if real is None else real + part_r
                imag = part_i if imag is None else imag + part_i
            for k in range(NX):
                ost[slot, k, 2 * gamma : 2 * gamma + 1, :] = real[k : k + 1]
                ost[slot, k, 2 * gamma + 1 : 2 * gamma + 2, :] = imag[k : k + 1]

    def total_to(v):
        return push(tm, tm, ms.at[v], tr, along_z(v))

    upward = w < HALF

    def relay_up(act):
        @pl.when(upward & (w > 0) & (lax.rem(w, STEP) == 0))
        def _():
            far = jnp.minimum(w + STEP, HALF - 1)
            loop(0, far - w, lambda i: act(far - i))

    def relay(act):
        relay_up(act)
        for hub_w, first, stop in DOWN:

            @pl.when(w == hub_w)
            def _():
                loop(first, stop, act)

    def late_to(v):
        tiles = p1g.at[pl.ds(HALF, NZ - HALF)]
        return push(tiles, tiles, ls.at[v], lr, along_z(v))

    def spread_tiles():
        flat = p1g[...].astype(F32).reshape(NZ * 8, 128)
        p1f[8 : NZ * 8] = flat[0 : NZ * 8 - 8]
        p1f[0:8] = flat[NZ * 8 - 8 :]

    def relay_root(act):
        for v in ROOT_UP + ROOT_DOWN:
            act(v)

    def rows_to_last(k):
        return push(
            ost.at[0, k], orv.at[x], o0s.at[k], ors.at[x], {"space_0": k, "space_1": zof(last)}
        )

    def rows_to_x(d):
        k = lax.rem(x + d, NX)
        return push(ost.at[1, k], orv.at[x], os_.at[d - 1], ors.at[x], along_x(d))

    def rows_from(k):
        push(ost.at[1, k], orv.at[k], os_.at[0], ors.at[k], along_x(1)).wait_recv()

    @pl.when(w == 0)
    def _():
        for v in ROOT_UP:
            late_to(v).start()
        prepare(0)
        prepare(1)
        spread_tiles()

        loop(NZ - LAG, NZ, add_direct)
        tm[...] = s1[...]
        for v in ROOT_UP:
            total_to(v).start()
        project(0)
        for k in range(NX):
            rows_to_last(k).start()
        for v in ROOT_DOWN:
            total_to(v).start()

    @pl.when((w > 0) & (w < last))
    def _():
        prepare(1)

    @pl.when((w > 0) & upward)
    def _():
        late_to(w).wait_recv()

    relay_up(lambda v: late_to(v).start())

    @pl.when((w > 0) & (w < last))
    def _():
        total_to(w).wait_recv()

    relay(lambda v: total_to(v).start())

    @pl.when((w > 0) & (w < last))
    def _():
        spread_tiles()

    @pl.when(w < last)
    def _():
        project(1)
        for d in (2, 1, 3):
            rows_to_x(d).start()

    @pl.when(w < last)
    def _():
        for d in (1, 3, 2):
            rows_from(lax.rem(x + d, NX))
        orv[x] = ost[1, x]

    @pl.when(w == last)
    def _():
        for k in range(NX):
            rows_from(k)

    out[...] = orv[0] + orv[1] + orv[2] + orv[3]

    for copy in x_copies + p0_copies:
        copy.wait_send()

    @pl.when(w > 0)
    def _():
        to_parent().wait_send()
        left_rows_root().wait_send()

    @pl.when(w > 0)
    def _():
        right_tile(0).wait_send()

    loop(direct, w, lambda v: right_tile(v).wait_send())
    loop(1, w, lambda v: left_row(v).wait_send())

    def answered(v):
        right_tile(v).wait_send()
        left_row(v).wait_send()

    loop(w + 1, last, answered)

    @pl.when(w == 0)
    def _():
        relay_root(lambda v: total_to(v).wait_send())
        for v in ROOT_UP:
            late_to(v).wait_send()

        for k in range(NX):
            rows_to_last(k).wait_send()

    relay(lambda v: total_to(v).wait_send())
    relay_up(lambda v: late_to(v).wait_send())

    @pl.when(w < last)
    def _():
        for d in (2, 1, 3):
            rows_to_x(d).wait_send()


def on_device(eigvecs, perambulator, momenta, source_slots, gamma_columns, gamma_phases):
    local_sites = eigvecs.shape[1]
    eig_count = eigvecs.shape[4]
    store_count = perambulator.shape[1]
    total_sites = local_sites * lax.axis_size(SPACE)
    extent_x = total_sites // (LY * LZ)
    lines = local_sites // LZ
    rows = LZ * 6
    assert local_sites == lines * LZ and eig_count == NX * NZ == 128 and lines <= 8
    count = gamma_columns.shape[0]
    vmem = lambda shape, dtype=F32: pltpu.VMEM(shape, dtype)
    dma = lambda n: pltpu.SemaphoreType.DMA((n,))

    meson = pl.pallas_call(
        functools.partial(
            kernel, lines, rows, extent_x, 1.0 / math.sqrt(12.0 * total_sites), count
        ),
        out_shape=pltpu.VMEM((2 * count, 128), F32),
        in_specs=[pl.BlockSpec(memory_space=pltpu.HBM)] * 6,
        out_specs=pl.BlockSpec(memory_space=pltpu.VMEM),
        scratch_shapes=[
            pltpu.SMEM(momenta.shape, jnp.int32),
            pltpu.SMEM(source_slots.shape, jnp.int32),
            pltpu.SMEM(gamma_columns.shape[::-1], jnp.int32),
            pltpu.SMEM(gamma_phases.shape[::-1], jnp.int32),
            vmem((lines * rows, 128), BF),
            vmem((store_count, 8, 128), BF),
            vmem((rows, 128)),
            vmem((rows, 128)),
            vmem((8, 128)),
            vmem((8, 128)),
            vmem((NX, 64, 128)),
            vmem((3, 64, 128)),
            vmem((64, 128)),
            vmem((64, 128), WIRE),
            vmem((NZ, 64, 128), WIRE),
            vmem((64, 128)),
            vmem((NX, 8, 128), BF),
            vmem((NZ, 1, 128)),
            vmem((NZ, 2, 1, 128)),
            vmem((NZ, 8, 128), BF),
            vmem((NZ * 8, 128)),
            vmem((2, 32, 128), BF),
            vmem((4, 2, 16, 128)),
            vmem((2, NX, 2 * count, 128)),
            vmem((NX, 2 * count, 128)),
            dma(6),
            pltpu.SemaphoreType.REGULAR,
            dma(3), dma(3), dma(3), dma(3),
            dma(NZ), dma(NZ), dma(NZ), dma(NZ), dma(NZ + 1), dma(NZ),
            pltpu.SemaphoreType.DMA,
            dma(NZ), pltpu.SemaphoreType.DMA,
            dma(3), dma(NX), dma(NX),
        ],
        compiler_params=pltpu.CompilerParams(
            collective_id=0, has_side_effects=True, vmem_limit_bytes=63043328
        ),
        name="meson",
    )(
        eigvecs.reshape(local_sites * 6, eig_count),
        perambulator.reshape(store_count, 8, eig_count),
        momenta,
        source_slots,
        gamma_columns.T,
        gamma_phases.T,
    )
    return meson.reshape(1, 1, 1, count, 2, eig_count)


def solution(mesh):
    split_mesh = Mesh(
        mesh.devices.reshape(mesh.shape["cfg"], NX, NZ, mesh.shape["tm"]),
        ("cfg", "space_0", "space_1", "tm"),
    )
    placed = (
        P(("cfg", "tm"), SPACE, None, None, None),
        P(("cfg", "tm"), None, None, None, SPACE, None),
        P(),
        P(),
        P(),
        P(),
    )
    return jax.shard_map(
        on_device,
        mesh=split_mesh,
        in_specs=placed,
        out_specs=P(("cfg", "tm"), SPACE, None, None, None, None),
        check_vma=False,
    )
```

```python
import functools
import math

import jax
import jax.numpy as jnp
from jax import lax
from jax.experimental import pallas as pl
from jax.experimental.pallas import tpu as pltpu
from jax.sharding import Mesh
from jax.sharding import PartitionSpec as P

LY = 48
LZ = 48
NX = 4
NZ = 32
HALF = 17
STEP = 4
LAG = 6
HUBS = ((4, 5, 9), (9, 10, 14), (19, 17, 19), (22, 20, 22), (25, 23, 25), (28, 26, 28))
ROOT_UP = (4, 1, 2, 3)
ROOT_DOWN = (22, 28)
DOWN = ((28, 24, 28), (28, 29, 31), (22, 17, 22), (22, 23, 24))
SPACE = ("space_0", "space_1")
BF = jnp.bfloat16
F32 = jnp.float32
WIRE = BF
MESH = pl.DeviceIdType.MESH


def iota(shape, dim):
    return lax.broadcasted_iota(jnp.int32, shape, dim)


def mm(a, b, dims):
    return lax.dot_general(a, b, (dims, ((), ())), preferred_element_type=F32)


def part_turns(momentum, coord, extent):
    product = (momentum * coord).astype(F32)
    return product / extent - jnp.floor(product / extent)


def wave_overlap(eig, tab_c, tab_s, line_c, line_s, lines, rows):
    even = (iota((rows, 128), 0) & 1) == 0
    total = None
    for line in range(lines):
        block = eig[pl.ds(line * rows, rows), :]
        wide = block.astype(F32)
        other = jnp.where(even, pltpu.roll(wide, rows - 1, 0), -pltpu.roll(wide, 1, 0))
        ca = line_c[line : line + 1, :]
        sa = line_s[line : line + 1, :]
        cb = tab_c[...]
        sb = tab_s[...]
        c = ca * cb - sa * sb
        s = sa * cb + ca * sb
        first = (c * wide + s * other).astype(BF)
        second = (s * wide - c * other).astype(BF)
        turned = jnp.concatenate([first, second], axis=1)
        product = mm(block, turned, ((0,), (0,)))
        total = product if total is None else total + product
    return total


def split(value):
    high = value.astype(BF)
    return high, (value - high.astype(F32)).astype(BF)


def kernel(
    lines, rows, extent_x, factor, count,
    eig_hbm, per_hbm, mom_hbm, slots_hbm, col_hbm, pha_hbm,
    out,
    momenta, slots, columns, phases,
    eig, per, tab_c, tab_s, line_c, line_s,
    mst, xr, s1, s1b, mr, tm, p0x, gst, p0g, p1g, p1f, lft, ast, ost, orv,
    loc_sem, ready, pr, xs, xrs, hs, hrs, p0s, p0r, p1s, p1r, ms, mrs, tr, ls, lr, os_, ors, o0s,
):
    x = lax.axis_index("space_0")
    z = lax.axis_index("space_1")
    w = lax.rem(z + (NZ - 1), NZ)
    last = NZ - 1

    def zof(v):
        return lax.rem(v + 1, NZ)

    def along_x(d):
        return {"space_0": lax.rem(x + d, NX), "space_1": z}

    def along_z(v):
        return {"space_0": x, "space_1": zof(v)}

    def push(src, dst, send, recv, device):
        return pltpu.make_async_remote_copy(
            src_ref=src, dst_ref=dst, send_sem=send, recv_sem=recv,
            device_id=device, device_id_type=MESH,
        )

    def loop(lower, upper, body):
        def step(v, carry):
            body(v)
            return carry

        lax.fori_loop(lower, upper, step, 0)

    pairs = (
        (mom_hbm, momenta), (eig_hbm, eig), (slots_hbm, slots),
        (per_hbm, per), (col_hbm, columns), (pha_hbm, phases),
    )
    loads = [pltpu.make_async_copy(a, b, loc_sem.at[k]) for k, (a, b) in enumerate(pairs)]
    for load in loads:
        load.start()
    load_mom, load_eig, load_slots, load_per, load_col, load_pha = loads

    barrier = pltpu.get_barrier_semaphore()
    for d in range(1, NX):
        pl.semaphore_signal(barrier, inc=1, device_id=along_x(d), device_id_type=MESH)

    def greet(v):
        pl.semaphore_signal(barrier, inc=1, device_id=along_z(v), device_id_type=MESH)

    loop(w + 1, NZ, greet)

    load_mom.wait()
    inner = iota((rows, 128), 0) // 6
    angle = (2.0 * math.pi) * part_turns(momenta[0, 2], inner, LZ)
    tab_c[...] = jnp.cos(angle)
    tab_s[...] = jnp.sin(angle)
    line_ids = (x * NZ + z) * lines + iota((8, 128), 0)
    turns = part_turns(momenta[0, 0], line_ids // LY, extent_x) + part_turns(
        momenta[0, 1], lax.rem(line_ids, LY), LY
    )
    angle = (2.0 * math.pi) * turns
    line_c[...] = jnp.cos(angle)
    line_s[...] = jnp.sin(angle)

    load_slots.wait()
    load_per.wait()
    p0x[x] = per[slots[0]]
    p1g[w] = per[slots[1]]
    load_col.wait()
    load_pha.wait()
    pl.semaphore_wait(barrier, w + (NX - 1))

    for hub, first, stop in HUBS:
        if hub > first:

            @pl.when(w == hub)
            def _():
                def tell(v):
                    pl.semaphore_signal(ready, inc=1, device_id=along_z(v), device_id_type=MESH)

                loop(first, stop, tell)

    p0_copies = []
    for k, d in enumerate((2, 1, 3)):
        copy = push(p0x.at[x], p0x.at[x], hs.at[k], hrs.at[k], along_x(d))
        copy.start()
        p0_copies.append(copy)
    def right_tile(v):
        return push(p1g.at[w], p1g.at[w], p1s.at[v], p1r.at[w], along_z(v))

    def left_row(v):
        return push(
            gst.at[pl.ds(zof(v), 1)], p0g.at[w, pl.ds(1, 1)], p0s.at[v], p0r.at[w], along_z(v)
        )

    def left_rows_root(recv):
        return push(gst.at[pl.ds(0, 2)], p0g.at[w], p0s.at[0], recv, along_z(0))

    def tile_root(recv):
        return push(p1g.at[w], p1g.at[w], p1s.at[0], recv, along_z(0))

    early = (w > 0) & (w < HALF)

    direct = jnp.where(w < HALF, 1, HALF)

    @pl.when(early)
    def _():
        tile_root(p1r.at[w]).start()

    @pl.when(w >= HALF)
    def _():
        tile_root(pr.at[0]).start()

    load_eig.wait()
    total = wave_overlap(eig, tab_c, tab_s, line_c, line_s, lines, rows)
    mst[:, 0:32] = total[:, 0:128].reshape(NX, 32, 128)
    mst[:, 32:64] = total[:, 128:256].reshape(NX, 32, 128)
    x_copies = []
    for k, d in enumerate((2, 1, 3)):
        copy = push(mst.at[lax.rem(x + d, NX)], xr.at[k], xs.at[k], xrs.at[k], along_x(d))
        copy.start()
        x_copies.append(copy)
    loop(direct, w, lambda v: right_tile(v).start())
    for copy in p0_copies:
        copy.wait_recv()
    row = iota((128, 32), 0)
    source = (row >> 5) * 8 + ((row >> 2) & 3) * 2 + ((row >> 4) & 1)
    spread = jnp.where(iota((128, 32), 1) == source, 1.0, 0.0).astype(BF)
    tiles = p0x[...].astype(F32).reshape(32, 128).astype(BF)
    spread = mm(spread, tiles, ((1,), (0,)))
    mine = (iota((128, 128), 1) >> 5) == (iota((128, 128), 0) & 3)
    spread = jnp.where(mine, spread, 0.0).astype(BF)
    comb = jnp.where((iota((32, 128), 1) & 31) == iota((32, 128), 0), 1.0, 0.0).astype(BF)
    gst[...] = mm(comb, spread, ((1,), (1,))).reshape(32, 1, 128)

    @pl.when(w > 0)
    def _():
        p0g[w, 1] = gst[z]

    @pl.when(early)
    def _():
        left_rows_root(p0r.at[w]).start()

    @pl.when(w >= HALF)
    def _():
        left_rows_root(pr.at[1]).start()

    @pl.when(w == 0)
    def _():
        p0g[w] = gst[0:2]

    loop(1, w, lambda v: left_row(v).start())

    for copy in x_copies:
        copy.wait_recv()
    value = mst[x] + xr[0] + xr[1] + xr[2]
    s1[...] = value

    def parent_of(v):
        parent = 0
        for hub, first, stop in HUBS:
            parent = jnp.where((v >= first) & (v < stop), hub, parent)
        return parent

    def to_parent():
        return push(s1b, mr.at[w], ms.at[NZ], mrs.at[w], along_z(parent_of(w)))

    def add(v):
        push(s1b, mr.at[v], ms.at[NZ], mrs.at[v], along_z(v)).wait_recv()
        s1[...] += mr[v].astype(F32)

    for hub, first, stop in HUBS:

        @pl.when(w == hub)
        def _():
            loop(first, stop, add)

        if hub > first:

            @pl.when((w >= first) & (w < stop))
            def _():
                pl.semaphore_wait(ready, 1)

    s1b[...] = s1[...].astype(WIRE)

    @pl.when(w > 0)
    def _():
        to_parent().start()

    def add_direct(v):
        @pl.when(parent_of(v) == 0)
        def _():
            add(v)

    def late_to(v):
        tiles = p1g.at[pl.ds(HALF, NZ - HALF)]
        return push(tiles, tiles, ls.at[v], lr, along_z(v))

    def answer(v):
        right_tile(v).start()
        left_row(v).start()

    def landed_tile(v):
        push(p1g.at[v], p1g.at[v], p1s.at[v], p1r.at[v], along_z(v)).wait_recv()

    def landed(v):

        @pl.when((v < HALF) | (w >= HALF))
        def _():
            landed_tile(v)

        push(
            gst.at[pl.ds(0, 1)], p0g.at[v, pl.ds(1, 1)], p0s.at[v], p0r.at[v], along_z(v)
        ).wait_recv()

    def landed_root(v):
        landed_tile(v)
        push(gst.at[pl.ds(0, 2)], p0g.at[v], p0s.at[v], p0r.at[v], along_z(v)).wait_recv()

    @pl.when(w == 0)
    def _():
        def meet(v):
            landed_root(v)
            answer(v)

            @pl.when(v > LAG)
            def _():
                add_direct(v - LAG)

        loop(1, HALF, meet)
        tiles = p1g.at[pl.ds(HALF, NZ - HALF)]
        push(tiles, tiles, p1s.at[0], pr.at[0], along_z(1)).wait_recv()
        for v in ROOT_UP:
            late_to(v).start()
        some = p0g.at[pl.ds(HALF, NZ - HALF)]
        push(some, some, p0s.at[0], pr.at[1], along_z(1)).wait_recv()

    @pl.when((w > 0) & (w < last))
    def _():
        def meet(v):
            landed(v)
            answer(v)

        loop(w + 1, last, meet)
        landed(last)
        loop(0, w, landed)

    def prepare(slot):
        rows_ = p0g[:, slot].reshape(32, 128).astype(BF)
        places = lax.rem(iota((32, 128), 0) + 1, NZ)
        placed = jnp.where((iota((32, 128), 1) & 31) == places, 1.0, 0.0).astype(BF)
        gathered = mm(rows_, placed, ((0,), (0,)))
        mine_ = (iota((128, 128), 1) >> 5) == (iota((128, 128), 0) >> 5)
        lft[slot] = jnp.where(mine_, gathered, 0.0).reshape(4, 32, 128).sum(axis=0).astype(BF)

    def project(slot):
        left = lft[slot]
        halves = []
        for part in (0, 1):
            high, low = split(tm[32 * part : 32 * part + 32])
            halves.append(mm(left, high, ((1,), (1,))) + mm(left, low, ((1,), (1,))))
        with_real, with_imag = halves
        x_real = with_real[0:16] + with_imag[16:32]
        x_imag = with_imag[0:16] - with_real[16:32]
        high, low = split(jnp.concatenate([x_real, x_imag], axis=0))
        stacked = jnp.concatenate([high, low], axis=0)
        for spin in range(4):
            made = []
            for part in (0, 1):
                right = p1f[pl.ds(2 * spin + part, NZ, stride=8), :].astype(BF)
                full = mm(stacked, right, ((1,), (0,)))
                made.append(full[0:32] + full[32:64])
            ast[spin, 0] = made[0][0:16] - made[1][16:32]
            ast[spin, 1] = made[1][0:16] + made[0][16:32]
        for gamma in range(count):
            real = imag = None
            for spin in range(4):
                col = columns[spin, gamma]
                power = phases[spin, gamma]
                cr = jnp.where(power == 0, factor, 0.0) - jnp.where(power == 2, factor, 0.0)
                ci = jnp.where(power == 1, factor, 0.0) - jnp.where(power == 3, factor, 0.0)
                a_real = ast[col, 0, 4 * spin : 4 * spin + 4, :]
                a_imag = ast[col, 1, 4 * spin : 4 * spin + 4, :]
                part_r = cr * a_real - ci * a_imag
                part_i = cr * a_imag + ci * a_real
                real = part_r if real is None else real + part_r
                imag = part_i if imag is None else imag + part_i
            for k in range(NX):
                ost[slot, k, 2 * gamma : 2 * gamma + 1, :] = real[k : k + 1]
                ost[slot, k, 2 * gamma + 1 : 2 * gamma + 2, :] = imag[k : k + 1]

    def total_to(v):
        return push(tm, tm, ms.at[v], tr, along_z(v))

    upward = w < HALF

    def relay_up(act):
        @pl.when(upward & (w > 0) & (lax.rem(w, STEP) == 0))
        def _():
            far = jnp.minimum(w + STEP, HALF - 1)
            loop(0, far - w, lambda i: act(far - i))

    def relay(act):
        relay_up(act)
        for hub_w, first, stop in DOWN:

            @pl.when(w == hub_w)
            def _():
                loop(first, stop, act)

    def spread_tiles():
        flat = p1g[...].astype(F32).reshape(NZ * 8, 128)
        p1f[8 : NZ * 8] = flat[0 : NZ * 8 - 8]
        p1f[0:8] = flat[NZ * 8 - 8 :]

    def relay_root(act):
        for v in ROOT_UP + ROOT_DOWN:
            act(v)

    def rows_to_last(k):
        return push(
            ost.at[0, k], orv.at[x], o0s.at[k], ors.at[x], {"space_0": k, "space_1": zof(last)}
        )

    def rows_to_x(d):
        k = lax.rem(x + d, NX)
        return push(ost.at[1, k], orv.at[x], os_.at[d - 1], ors.at[x], along_x(d))

    def rows_from(k):
        push(ost.at[1, k], orv.at[k], os_.at[0], ors.at[k], along_x(1)).wait_recv()

    @pl.when(w == 0)
    def _():
        prepare(0)
        prepare(1)
        spread_tiles()

        loop(HALF - LAG, HALF, add_direct)
        loop(HALF, last, answer)
        loop(HALF, NZ, add_direct)
        tm[...] = s1[...]
        for v in ROOT_UP:
            total_to(v).start()
        project(0)
        for k in range(NX):
            rows_to_last(k).start()
        for v in ROOT_DOWN:
            total_to(v).start()

    @pl.when((w > 0) & (w < last))
    def _():
        prepare(1)

    @pl.when((w > 0) & upward)
    def _():
        late_to(w).wait_recv()

    relay_up(lambda v: late_to(v).start())

    @pl.when((w > 0) & (w < last))
    def _():
        total_to(w).wait_recv()

    relay(lambda v: total_to(v).start())

    @pl.when((w > 0) & (w < last))
    def _():
        spread_tiles()

    @pl.when(w < last)
    def _():
        project(1)
        for d in (2, 1, 3):
            rows_to_x(d).start()

    @pl.when(w < last)
    def _():
        for d in (1, 3, 2):
            rows_from(lax.rem(x + d, NX))
        orv[x] = ost[1, x]

    @pl.when(w == last)
    def _():
        for k in range(NX):
            rows_from(k)

    out[...] = orv[0] + orv[1] + orv[2] + orv[3]

    for copy in x_copies + p0_copies:
        copy.wait_send()

    @pl.when(w > 0)
    def _():
        to_parent().wait_send()
        left_rows_root(pr.at[1]).wait_send()

    @pl.when(w > 0)
    def _():
        tile_root(pr.at[0]).wait_send()

    loop(direct, w, lambda v: right_tile(v).wait_send())
    loop(1, w, lambda v: left_row(v).wait_send())

    def answered(v):
        right_tile(v).wait_send()
        left_row(v).wait_send()

    loop(w + 1, last, answered)

    @pl.when(w == 0)
    def _():
        relay_root(lambda v: total_to(v).wait_send())
        for v in ROOT_UP:
            late_to(v).wait_send()

        for k in range(NX):
            rows_to_last(k).wait_send()

    relay(lambda v: total_to(v).wait_send())
    relay_up(lambda v: late_to(v).wait_send())

    @pl.when(w < last)
    def _():
        for d in (2, 1, 3):
            rows_to_x(d).wait_send()


def on_device(eigvecs, perambulator, momenta, source_slots, gamma_columns, gamma_phases):
    local_sites = eigvecs.shape[1]
    eig_count = eigvecs.shape[4]
    store_count = perambulator.shape[1]
    total_sites = local_sites * lax.axis_size(SPACE)
    extent_x = total_sites // (LY * LZ)
    lines = local_sites // LZ
    rows = LZ * 6
    assert local_sites == lines * LZ and eig_count == NX * NZ == 128 and lines <= 8
    count = gamma_columns.shape[0]
    vmem = lambda shape, dtype=F32: pltpu.VMEM(shape, dtype)
    dma = lambda n: pltpu.SemaphoreType.DMA((n,))

    meson = pl.pallas_call(
        functools.partial(
            kernel, lines, rows, extent_x, 1.0 / math.sqrt(12.0 * total_sites), count
        ),
        out_shape=pltpu.VMEM((2 * count, 128), F32),
        in_specs=[pl.BlockSpec(memory_space=pltpu.HBM)] * 6,
        out_specs=pl.BlockSpec(memory_space=pltpu.VMEM),
        scratch_shapes=[
            pltpu.SMEM(momenta.shape, jnp.int32),
            pltpu.SMEM(source_slots.shape, jnp.int32),
            pltpu.SMEM(gamma_columns.shape[::-1], jnp.int32),
            pltpu.SMEM(gamma_phases.shape[::-1], jnp.int32),
            vmem((lines * rows, 128), BF),
            vmem((store_count, 8, 128), BF),
            vmem((rows, 128)),
            vmem((rows, 128)),
            vmem((8, 128)),
            vmem((8, 128)),
            vmem((NX, 64, 128)),
            vmem((3, 64, 128)),
            vmem((64, 128)),
            vmem((64, 128), WIRE),
            vmem((NZ, 64, 128), WIRE),
            vmem((64, 128)),
            vmem((NX, 8, 128), BF),
            vmem((NZ, 1, 128)),
            vmem((NZ, 2, 1, 128)),
            vmem((NZ, 8, 128), BF),
            vmem((NZ * 8, 128)),
            vmem((2, 32, 128), BF),
            vmem((4, 2, 16, 128)),
            vmem((2, NX, 2 * count, 128)),
            vmem((NX, 2 * count, 128)),
            dma(6),
            pltpu.SemaphoreType.REGULAR,
            dma(2),
            dma(3), dma(3), dma(3), dma(3),
            dma(NZ), dma(NZ), dma(NZ), dma(NZ), dma(NZ + 1), dma(NZ),
            pltpu.SemaphoreType.DMA,
            dma(NZ), pltpu.SemaphoreType.DMA,
            dma(3), dma(NX), dma(NX),
        ],
        compiler_params=pltpu.CompilerParams(
            collective_id=0, has_side_effects=True, vmem_limit_bytes=63043328
        ),
        name="meson",
    )(
        eigvecs.reshape(local_sites * 6, eig_count),
        perambulator.reshape(store_count, 8, eig_count),
        momenta,
        source_slots,
        gamma_columns.T,
        gamma_phases.T,
    )
    return meson.reshape(1, 1, 1, count, 2, eig_count)


def solution(mesh):
    split_mesh = Mesh(
        mesh.devices.reshape(mesh.shape["cfg"], NX, NZ, mesh.shape["tm"]),
        ("cfg", "space_0", "space_1", "tm"),
    )
    placed = (
        P(("cfg", "tm"), SPACE, None, None, None),
        P(("cfg", "tm"), None, None, None, SPACE, None),
        P(),
        P(),
        P(),
        P(),
    )
    return jax.shard_map(
        on_device,
        mesh=split_mesh,
        in_specs=placed,
        out_specs=P(("cfg", "tm"), SPACE, None, None, None, None),
        check_vma=False,
    )
```

```python
import functools
import math

import jax
import jax.numpy as jnp
from jax import lax
from jax.experimental import pallas as pl
from jax.experimental.pallas import tpu as pltpu
from jax.sharding import Mesh
from jax.sharding import PartitionSpec as P

LY = 48
LZ = 48
NX = 4
NZ = 32
HALF = 17
STEP = 4
LAG = 6
HUBS = ((4, 5, 9), (9, 10, 14), (19, 17, 19), (22, 20, 22), (25, 23, 25))
ROOT_UP = (4, 2, 3)
ROOT_DOWN = (22, 28)
DOWN = ((28, 24, 28), (28, 29, 31), (22, 17, 22), (22, 23, 24))
SPACE = ("space_0", "space_1")
BF = jnp.bfloat16
F32 = jnp.float32
WIRE = BF
MESH = pl.DeviceIdType.MESH


def iota(shape, dim):
    return lax.broadcasted_iota(jnp.int32, shape, dim)


def mm(a, b, dims):
    return lax.dot_general(a, b, (dims, ((), ())), preferred_element_type=F32)


def part_turns(momentum, coord, extent):
    product = (momentum * coord).astype(F32)
    return product / extent - jnp.floor(product / extent)


def wave_overlap(eig, tab_c, tab_s, line_c, line_s, lines, rows):
    even = (iota((rows, 128), 0) & 1) == 0
    total = None
    for line in range(lines):
        block = eig[pl.ds(line * rows, rows), :]
        wide = block.astype(F32)
        other = jnp.where(even, pltpu.roll(wide, rows - 1, 0), -pltpu.roll(wide, 1, 0))
        ca = line_c[line : line + 1, :]
        sa = line_s[line : line + 1, :]
        cb = tab_c[...]
        sb = tab_s[...]
        c = ca * cb - sa * sb
        s = sa * cb + ca * sb
        first = (c * wide + s * other).astype(BF)
        second = (s * wide - c * other).astype(BF)
        turned = jnp.concatenate([first, second], axis=1)
        product = mm(block, turned, ((0,), (0,)))
        total = product if total is None else total + product
    return total


def split(value):
    high = value.astype(BF)
    return high, (value - high.astype(F32)).astype(BF)


def kernel(
    lines, rows, extent_x, factor, count,
    eig_hbm, per_hbm, mom_hbm, slots_hbm, col_hbm, pha_hbm,
    out,
    momenta, slots, columns, phases,
    eig, per, tab_c, tab_s, line_c, line_s,
    mst, xr, s1, s1b, mr, tm, p0x, gst, p0g, p1g, p1f, lft, ast, ost, orv,
    loc_sem, ready, pr, xs, xrs, hs, hrs, p0s, p0r, p1s, p1r, ms, mrs, tr, ls, lr, os_, ors, o0s, o2s,
):
    x = lax.axis_index("space_0")
    z = lax.axis_index("space_1")
    w = lax.rem(z + (NZ - 1), NZ)
    last = NZ - 1

    def zof(v):
        return lax.rem(v + 1, NZ)

    def along_x(d):
        return {"space_0": lax.rem(x + d, NX), "space_1": z}

    def along_z(v):
        return {"space_0": x, "space_1": zof(v)}

    def push(src, dst, send, recv, device):
        return pltpu.make_async_remote_copy(
            src_ref=src, dst_ref=dst, send_sem=send, recv_sem=recv,
            device_id=device, device_id_type=MESH,
        )

    def loop(lower, upper, body):
        def step(v, carry):
            body(v)
            return carry

        lax.fori_loop(lower, upper, step, 0)

    pairs = (
        (mom_hbm, momenta), (eig_hbm, eig), (slots_hbm, slots),
        (per_hbm, per), (col_hbm, columns), (pha_hbm, phases),
    )
    loads = [pltpu.make_async_copy(a, b, loc_sem.at[k]) for k, (a, b) in enumerate(pairs)]
    for load in loads:
        load.start()
    load_mom, load_eig, load_slots, load_per, load_col, load_pha = loads

    barrier = pltpu.get_barrier_semaphore()
    for d in range(1, NX):
        pl.semaphore_signal(barrier, inc=1, device_id=along_x(d), device_id_type=MESH)

    def greet(v):
        pl.semaphore_signal(barrier, inc=1, device_id=along_z(v), device_id_type=MESH)

    loop(w + 1, NZ, greet)

    load_mom.wait()
    inner = iota((rows, 128), 0) // 6
    angle = (2.0 * math.pi) * part_turns(momenta[0, 2], inner, LZ)
    tab_c[...] = jnp.cos(angle)
    tab_s[...] = jnp.sin(angle)
    line_ids = (x * NZ + z) * lines + iota((8, 128), 0)
    turns = part_turns(momenta[0, 0], line_ids // LY, extent_x) + part_turns(
        momenta[0, 1], lax.rem(line_ids, LY), LY
    )
    angle = (2.0 * math.pi) * turns
    line_c[...] = jnp.cos(angle)
    line_s[...] = jnp.sin(angle)

    load_slots.wait()
    load_per.wait()
    p0x[x] = per[slots[0]]
    p1g[w] = per[slots[1]]
    load_col.wait()
    load_pha.wait()
    pl.semaphore_wait(barrier, w + (NX - 1))

    for hub, first, stop in HUBS:
        if hub > first:

            @pl.when(w == hub)
            def _():
                def tell(v):
                    pl.semaphore_signal(ready, inc=1, device_id=along_z(v), device_id_type=MESH)

                loop(first, stop, tell)

    p0_copies = []
    for k, d in enumerate((2, 1, 3)):
        copy = push(p0x.at[x], p0x.at[x], hs.at[k], hrs.at[k], along_x(d))
        copy.start()
        p0_copies.append(copy)
    def right_tile(v):
        return push(p1g.at[w], p1g.at[w], p1s.at[v], p1r.at[w], along_z(v))

    def left_row(v):
        return push(
            gst.at[pl.ds(zof(v), 1)], p0g.at[w, pl.ds(1, 1)], p0s.at[v], p0r.at[w], along_z(v)
        )

    def left_rows_root(recv):
        return push(gst.at[pl.ds(0, 3)], p0g.at[w], p0s.at[0], recv, along_z(0))

    def tile_root(recv):
        return push(p1g.at[w], p1g.at[w], p1s.at[0], recv, along_z(0))

    early = (w > 0) & (w < HALF)

    direct = jnp.where(w < HALF, 1, HALF)

    @pl.when(early)
    def _():
        tile_root(p1r.at[w]).start()

    @pl.when(w >= HALF)
    def _():
        tile_root(pr.at[0]).start()

    load_eig.wait()
    total = wave_overlap(eig, tab_c, tab_s, line_c, line_s, lines, rows)
    mst[:, 0:32] = total[:, 0:128].reshape(NX, 32, 128)
    mst[:, 32:64] = total[:, 128:256].reshape(NX, 32, 128)
    x_copies = []
    for k, d in enumerate((2, 1, 3)):
        copy = push(mst.at[lax.rem(x + d, NX)], xr.at[k], xs.at[k], xrs.at[k], along_x(d))
        copy.start()
        x_copies.append(copy)
    loop(direct, w, lambda v: right_tile(v).start())
    for copy in p0_copies:
        copy.wait_recv()
    row = iota((128, 32), 0)
    source = (row >> 5) * 8 + ((row >> 2) & 3) * 2 + ((row >> 4) & 1)
    spread = jnp.where(iota((128, 32), 1) == source, 1.0, 0.0).astype(BF)
    tiles = p0x[...].astype(F32).reshape(32, 128).astype(BF)
    spread = mm(spread, tiles, ((1,), (0,)))
    mine = (iota((128, 128), 1) >> 5) == (iota((128, 128), 0) & 3)
    spread = jnp.where(mine, spread, 0.0).astype(BF)
    comb = jnp.where((iota((32, 128), 1) & 31) == iota((32, 128), 0), 1.0, 0.0).astype(BF)
    gst[...] = mm(comb, spread, ((1,), (1,))).reshape(32, 1, 128)

    @pl.when(w > 0)
    def _():
        p0g[w, 1] = gst[z]

    @pl.when(early)
    def _():
        left_rows_root(p0r.at[w]).start()

    @pl.when(w >= HALF)
    def _():
        left_rows_root(pr.at[1]).start()

    @pl.when(w == 0)
    def _():
        p0g[w] = gst[0:3]

    loop(1, w, lambda v: left_row(v).start())

    for copy in x_copies:
        copy.wait_recv()
    value = mst[x] + xr[0] + xr[1] + xr[2]
    s1[...] = value

    def parent_of(v):
        parent = 0
        for hub, first, stop in HUBS:
            parent = jnp.where((v >= first) & (v < stop), hub, parent)
        return parent

    def to_parent():
        return push(s1b, mr.at[w], ms.at[NZ], mrs.at[w], along_z(parent_of(w)))

    def add(v):
        push(s1b, mr.at[v], ms.at[NZ], mrs.at[v], along_z(v)).wait_recv()
        s1[...] += mr[v].astype(F32)

    for hub, first, stop in HUBS:

        @pl.when(w == hub)
        def _():
            loop(first, stop, add)

        if hub > first:

            @pl.when((w >= first) & (w < stop))
            def _():
                pl.semaphore_wait(ready, 1)

    s1b[...] = s1[...].astype(WIRE)

    @pl.when(w > 0)
    def _():
        to_parent().start()

    def add_direct(v):
        @pl.when(parent_of(v) == 0)
        def _():
            add(v)

    def late_to(v):
        tiles = p1g.at[pl.ds(HALF, NZ - HALF)]
        return push(tiles, tiles, ls.at[v], lr, along_z(v))

    def answer(v):
        right_tile(v).start()
        left_row(v).start()

    def landed_tile(v):
        push(p1g.at[v], p1g.at[v], p1s.at[v], p1r.at[v], along_z(v)).wait_recv()

    def landed(v):

        @pl.when((v < HALF) | (w >= HALF))
        def _():
            landed_tile(v)

        push(
            gst.at[pl.ds(0, 1)], p0g.at[v, pl.ds(1, 1)], p0s.at[v], p0r.at[v], along_z(v)
        ).wait_recv()

    def landed_root(v):
        landed_tile(v)
        push(gst.at[pl.ds(0, 3)], p0g.at[v], p0s.at[v], p0r.at[v], along_z(v)).wait_recv()

    @pl.when(w == 0)
    def _():
        def meet(v):
            landed_root(v)
            answer(v)

            @pl.when(v > LAG)
            def _():
                add_direct(v - LAG)

        loop(1, HALF, meet)
        tiles = p1g.at[pl.ds(HALF, NZ - HALF)]
        push(tiles, tiles, p1s.at[0], pr.at[0], along_z(1)).wait_recv()
        for v in ROOT_UP:
            late_to(v).start()
        some = p0g.at[pl.ds(HALF, NZ - HALF)]
        push(some, some, p0s.at[0], pr.at[1], along_z(1)).wait_recv()

    @pl.when((w > 0) & (w < last))
    def _():
        def meet(v):
            landed(v)
            answer(v)

        loop(w + 1, last, meet)
        landed(last)
        loop(0, w, landed)

    def prepare(slot):
        rows_ = p0g[:, slot].reshape(32, 128).astype(BF)
        places = lax.rem(iota((32, 128), 0) + 1, NZ)
        placed = jnp.where((iota((32, 128), 1) & 31) == places, 1.0, 0.0).astype(BF)
        gathered = mm(rows_, placed, ((0,), (0,)))
        mine_ = (iota((128, 128), 1) >> 5) == (iota((128, 128), 0) >> 5)
        lft[slot] = jnp.where(mine_, gathered, 0.0).reshape(4, 32, 128).sum(axis=0).astype(BF)

    def project(slot):
        left = lft[slot]
        halves = []
        for part in (0, 1):
            high, low = split(tm[32 * part : 32 * part + 32])
            halves.append(mm(left, high, ((1,), (1,))) + mm(left, low, ((1,), (1,))))
        with_real, with_imag = halves
        x_real = with_real[0:16] + with_imag[16:32]
        x_imag = with_imag[0:16] - with_real[16:32]
        high, low = split(jnp.concatenate([x_real, x_imag], axis=0))
        stacked = jnp.concatenate([high, low], axis=0)
        for spin in range(4):
            made = []
            for part in (0, 1):
                right = p1f[pl.ds(2 * spin + part, NZ, stride=8), :].astype(BF)
                full = mm(stacked, right, ((1,), (0,)))
                made.append(full[0:32] + full[32:64])
            ast[spin, 0] = made[0][0:16] - made[1][16:32]
            ast[spin, 1] = made[1][0:16] + made[0][16:32]
        for gamma in range(count):
            real = imag = None
            for spin in range(4):
                col = columns[spin, gamma]
                power = phases[spin, gamma]
                cr = jnp.where(power == 0, factor, 0.0) - jnp.where(power == 2, factor, 0.0)
                ci = jnp.where(power == 1, factor, 0.0) - jnp.where(power == 3, factor, 0.0)
                a_real = ast[col, 0, 4 * spin : 4 * spin + 4, :]
                a_imag = ast[col, 1, 4 * spin : 4 * spin + 4, :]
                part_r = cr * a_real - ci * a_imag
                part_i = cr * a_imag + ci * a_real
                real = part_r if real is None else real + part_r
                imag = part_i if imag is None else imag + part_i
            for k in range(NX):
                ost[slot, k, 2 * gamma : 2 * gamma + 1, :] = real[k : k + 1]
                ost[slot, k, 2 * gamma + 1 : 2 * gamma + 2, :] = imag[k : k + 1]

    def total_to(v):
        return push(tm, tm, ms.at[v], tr, along_z(v))

    upward = w < HALF

    def relay_up(act):
        @pl.when(upward & (w > 0) & (lax.rem(w, STEP) == 0))
        def _():
            far = jnp.minimum(w + STEP, HALF - 1)
            loop(0, far - w, lambda i: act(far - i))

    def relay(act):
        relay_up(act)
        for hub_w, first, stop in DOWN:

            @pl.when(w == hub_w)
            def _():
                loop(first, stop, act)

    def spread_tiles():
        flat = p1g[...].astype(F32).reshape(NZ * 8, 128)
        p1f[8 : NZ * 8] = flat[0 : NZ * 8 - 8]
        p1f[0:8] = flat[NZ * 8 - 8 :]

    def relay_root(act):
        for v in ROOT_UP + ROOT_DOWN:
            act(v)

    def rows_to_last(k):
        return push(
            ost.at[0, k], orv.at[x], o0s.at[k], ors.at[x], {"space_0": k, "space_1": zof(last)}
        )

    def rows_to_next(k):
        return push(
            ost.at[2, k], orv.at[x], o2s.at[k], ors.at[x], {"space_0": k, "space_1": zof(1)}
        )

    def rows_to_x(d):
        k = lax.rem(x + d, NX)
        return push(ost.at[1, k], orv.at[x], os_.at[d - 1], ors.at[x], along_x(d))

    def rows_from(k):
        push(ost.at[1, k], orv.at[k], os_.at[0], ors.at[k], along_x(1)).wait_recv()

    @pl.when(w == 0)
    def _():
        prepare(0)
        prepare(1)
        prepare(2)
        spread_tiles()

        loop(HALF - LAG, HALF, add_direct)
        loop(HALF, last, answer)
        loop(HALF, NZ, add_direct)
        tm[...] = s1[...]
        for v in ROOT_UP:
            total_to(v).start()
        project(0)
        for k in range(NX):
            rows_to_last(k).start()
        for v in ROOT_DOWN:
            total_to(v).start()

    @pl.when((w > 1) & (w < last))
    def _():
        prepare(1)

    @pl.when((w > 1) & upward)
    def _():
        late_to(w).wait_recv()

    relay_up(lambda v: late_to(v).start())

    @pl.when((w > 1) & (w < last))
    def _():
        total_to(w).wait_recv()

    relay(lambda v: total_to(v).start())

    @pl.when((w > 1) & (w < last))
    def _():
        spread_tiles()

    own = (w < last) & (w != 1)

    @pl.when(own)
    def _():
        project(1)
        for d in (2, 1, 3):
            rows_to_x(d).start()

    @pl.when(w == 0)
    def _():
        project(2)
        for k in range(NX):
            rows_to_next(k).start()

    for copy in x_copies + p0_copies:
        copy.wait_send()

    @pl.when(w > 0)
    def _():
        to_parent().wait_send()
        left_rows_root(pr.at[1]).wait_send()

    @pl.when(w > 0)
    def _():
        tile_root(pr.at[0]).wait_send()

    loop(direct, w, lambda v: right_tile(v).wait_send())
    loop(1, w, lambda v: left_row(v).wait_send())

    def answered(v):
        right_tile(v).wait_send()
        left_row(v).wait_send()

    loop(w + 1, last, answered)

    @pl.when(own)
    def _():
        for d in (1, 3, 2):
            rows_from(lax.rem(x + d, NX))
        orv[x] = ost[1, x]

    @pl.when(~own)
    def _():
        for k in range(NX):
            rows_from(k)

    out[...] = orv[0] + orv[1] + orv[2] + orv[3]

    @pl.when(w == 0)
    def _():
        relay_root(lambda v: total_to(v).wait_send())
        for v in ROOT_UP:
            late_to(v).wait_send()

        for k in range(NX):
            rows_to_last(k).wait_send()
            rows_to_next(k).wait_send()

    relay(lambda v: total_to(v).wait_send())
    relay_up(lambda v: late_to(v).wait_send())

    @pl.when(own)
    def _():
        for d in (2, 1, 3):
            rows_to_x(d).wait_send()


def on_device(eigvecs, perambulator, momenta, source_slots, gamma_columns, gamma_phases):
    local_sites = eigvecs.shape[1]
    eig_count = eigvecs.shape[4]
    store_count = perambulator.shape[1]
    total_sites = local_sites * lax.axis_size(SPACE)
    extent_x = total_sites // (LY * LZ)
    lines = local_sites // LZ
    rows = LZ * 6
    assert local_sites == lines * LZ and eig_count == NX * NZ == 128 and lines <= 8
    count = gamma_columns.shape[0]
    vmem = lambda shape, dtype=F32: pltpu.VMEM(shape, dtype)
    dma = lambda n: pltpu.SemaphoreType.DMA((n,))

    meson = pl.pallas_call(
        functools.partial(
            kernel, lines, rows, extent_x, 1.0 / math.sqrt(12.0 * total_sites), count
        ),
        out_shape=pltpu.VMEM((2 * count, 128), F32),
        in_specs=[pl.BlockSpec(memory_space=pltpu.HBM)] * 6,
        out_specs=pl.BlockSpec(memory_space=pltpu.VMEM),
        scratch_shapes=[
            pltpu.SMEM(momenta.shape, jnp.int32),
            pltpu.SMEM(source_slots.shape, jnp.int32),
            pltpu.SMEM(gamma_columns.shape[::-1], jnp.int32),
            pltpu.SMEM(gamma_phases.shape[::-1], jnp.int32),
            vmem((lines * rows, 128), BF),
            vmem((store_count, 8, 128), BF),
            vmem((rows, 128)),
            vmem((rows, 128)),
            vmem((8, 128)),
            vmem((8, 128)),
            vmem((NX, 64, 128)),
            vmem((3, 64, 128)),
            vmem((64, 128)),
            vmem((64, 128), WIRE),
            vmem((NZ, 64, 128), WIRE),
            vmem((64, 128)),
            vmem((NX, 8, 128), BF),
            vmem((NZ, 1, 128)),
            vmem((NZ, 3, 1, 128)),
            vmem((NZ, 8, 128), BF),
            vmem((NZ * 8, 128)),
            vmem((3, 32, 128), BF),
            vmem((4, 2, 16, 128)),
            vmem((3, NX, 2 * count, 128)),
            vmem((NX, 2 * count, 128)),
            dma(6),
            pltpu.SemaphoreType.REGULAR,
            dma(2),
            dma(3), dma(3), dma(3), dma(3),
            dma(NZ), dma(NZ), dma(NZ), dma(NZ), dma(NZ + 1), dma(NZ),
            pltpu.SemaphoreType.DMA,
            dma(NZ), pltpu.SemaphoreType.DMA,
            dma(3), dma(NX), dma(NX), dma(NX),
        ],
        compiler_params=pltpu.CompilerParams(
            collective_id=0, has_side_effects=True, vmem_limit_bytes=63043328
        ),
        name="meson",
    )(
        eigvecs.reshape(local_sites * 6, eig_count),
        perambulator.reshape(store_count, 8, eig_count),
        momenta,
        source_slots,
        gamma_columns.T,
        gamma_phases.T,
    )
    return meson.reshape(1, 1, 1, count, 2, eig_count)


def solution(mesh):
    split_mesh = Mesh(
        mesh.devices.reshape(mesh.shape["cfg"], NX, NZ, mesh.shape["tm"]),
        ("cfg", "space_0", "space_1", "tm"),
    )
    placed = (
        P(("cfg", "tm"), SPACE, None, None, None),
        P(("cfg", "tm"), None, None, None, SPACE, None),
        P(),
        P(),
        P(),
        P(),
    )
    return jax.shard_map(
        on_device,
        mesh=split_mesh,
        in_specs=placed,
        out_specs=P(("cfg", "tm"), SPACE, None, None, None, None),
        check_vma=False,
    )
```

```python
import functools
import math

import jax
import jax.numpy as jnp
from jax import lax
from jax.experimental import pallas as pl
from jax.experimental.pallas import tpu as pltpu
from jax.sharding import Mesh
from jax.sharding import PartitionSpec as P

LY = 48
LZ = 48
NX = 4
NZ = 32
HALF = 17
STEP = 4
LAG = 6
HUBS = ((4, 5, 9), (9, 10, 14), (19, 17, 19), (22, 20, 22), (25, 23, 25))
ROOT_UP = (4, 2, 3)
ROOT_DOWN = (22, 28)
DOWN = ((28, 24, 28), (28, 29, 31), (22, 17, 22), (22, 23, 24))
SPACE = ("space_0", "space_1")
BF = jnp.bfloat16
F32 = jnp.float32
WIRE = BF
MESH = pl.DeviceIdType.MESH


def iota(shape, dim):
    return lax.broadcasted_iota(jnp.int32, shape, dim)


def mm(a, b, dims):
    return lax.dot_general(a, b, (dims, ((), ())), preferred_element_type=F32)


def part_turns(momentum, coord, extent):
    product = (momentum * coord).astype(F32)
    return product / extent - jnp.floor(product / extent)


def wave_overlap(eig, tab_c, tab_s, line_c, line_s, lines, rows):
    even = (iota((rows, 128), 0) & 1) == 0
    total = None
    for line in range(lines):
        block = eig[pl.ds(line * rows, rows), :]
        wide = block.astype(F32)
        other = jnp.where(even, pltpu.roll(wide, rows - 1, 0), -pltpu.roll(wide, 1, 0))
        ca = line_c[line : line + 1, :]
        sa = line_s[line : line + 1, :]
        cb = tab_c[...]
        sb = tab_s[...]
        c = ca * cb - sa * sb
        s = sa * cb + ca * sb
        first = (c * wide + s * other).astype(BF)
        second = (s * wide - c * other).astype(BF)
        turned = jnp.concatenate([first, second], axis=1)
        product = mm(block, turned, ((0,), (0,)))
        total = product if total is None else total + product
    return total


def split(value):
    high = value.astype(BF)
    return high, (value - high.astype(F32)).astype(BF)


def kernel(
    lines, rows, extent_x, factor, count,
    eig_hbm, per_hbm, mom_hbm, slots_hbm, col_hbm, pha_hbm,
    out,
    momenta, slots, columns, phases,
    eig, per, tab_c, tab_s, line_c, line_s,
    mst, xr, s1, s1b, mr, tm, p0x, gst, p0g, p1g, p1f, lft, ast, ost, orv,
    loc_sem, ready, pr, xs, xrs, hs, hrs, p0s, p0r, p1s, p1r, ms, mrs, tr, ls, lr, os_, ors, o0s, o2s,
):
    x = lax.axis_index("space_0")
    z = lax.axis_index("space_1")
    w = lax.rem(z + (NZ - 1), NZ)
    last = NZ - 1

    def zof(v):
        return lax.rem(v + 1, NZ)

    def along_x(d):
        return {"space_0": lax.rem(x + d, NX), "space_1": z}

    def along_z(v):
        return {"space_0": x, "space_1": zof(v)}

    def push(src, dst, send, recv, device):
        return pltpu.make_async_remote_copy(
            src_ref=src, dst_ref=dst, send_sem=send, recv_sem=recv,
            device_id=device, device_id_type=MESH,
        )

    def loop(lower, upper, body):
        def step(v, carry):
            body(v)
            return carry

        lax.fori_loop(lower, upper, step, 0)

    pairs = (
        (mom_hbm, momenta), (eig_hbm, eig), (slots_hbm, slots),
        (per_hbm, per), (col_hbm, columns), (pha_hbm, phases),
    )
    loads = [pltpu.make_async_copy(a, b, loc_sem.at[k]) for k, (a, b) in enumerate(pairs)]
    for load in loads:
        load.start()
    load_mom, load_eig, load_slots, load_per, load_col, load_pha = loads

    barrier = pltpu.get_barrier_semaphore()
    for d in range(1, NX):
        pl.semaphore_signal(barrier, inc=1, device_id=along_x(d), device_id_type=MESH)

    def greet(v):
        pl.semaphore_signal(barrier, inc=1, device_id=along_z(v), device_id_type=MESH)

    loop(w + 1, NZ, greet)

    load_mom.wait()
    angle = (2.0 * math.pi) * part_turns(momenta[0, 2], iota((LZ, 128), 0), LZ)
    inner_c = jnp.cos(angle)
    inner_s = jnp.sin(angle)
    for k in range(6):
        tab_c[pl.ds(k, LZ, stride=6), :] = inner_c
        tab_s[pl.ds(k, LZ, stride=6), :] = inner_s
    line_ids = (x * NZ + z) * lines + iota((8, 128), 0)
    turns = part_turns(momenta[0, 0], line_ids // LY, extent_x) + part_turns(
        momenta[0, 1], lax.rem(line_ids, LY), LY
    )
    angle = (2.0 * math.pi) * turns
    line_c[...] = jnp.cos(angle)
    line_s[...] = jnp.sin(angle)

    load_slots.wait()
    load_per.wait()
    p0x[x] = per[slots[0]]
    p1g[w] = per[slots[1]]
    load_col.wait()
    load_pha.wait()
    pl.semaphore_wait(barrier, w + (NX - 1))

    for hub, first, stop in HUBS:
        if hub > first:

            @pl.when(w == hub)
            def _():
                def tell(v):
                    pl.semaphore_signal(ready, inc=1, device_id=along_z(v), device_id_type=MESH)

                loop(first, stop, tell)

    p0_copies = []
    for k, d in enumerate((2, 1, 3)):
        copy = push(p0x.at[x], p0x.at[x], hs.at[k], hrs.at[k], along_x(d))
        copy.start()
        p0_copies.append(copy)
    def right_tile(v):
        return push(p1g.at[w], p1g.at[w], p1s.at[v], p1r.at[w], along_z(v))

    def left_row(v):
        return push(
            gst.at[pl.ds(zof(v), 1)], p0g.at[w, pl.ds(1, 1)], p0s.at[v], p0r.at[w], along_z(v)
        )

    def left_rows_root(recv):
        return push(gst.at[pl.ds(0, 3)], p0g.at[w], p0s.at[0], recv, along_z(0))

    def tile_root(recv):
        return push(p1g.at[w], p1g.at[w], p1s.at[0], recv, along_z(0))

    early = (w > 0) & (w < HALF)

    direct = jnp.where(w < HALF, 1, HALF)

    @pl.when(early)
    def _():
        tile_root(p1r.at[w]).start()

    @pl.when(w >= HALF)
    def _():
        tile_root(pr.at[0]).start()

    load_eig.wait()
    total = wave_overlap(eig, tab_c, tab_s, line_c, line_s, lines, rows)
    mst[:, 0:32] = total[:, 0:128].reshape(NX, 32, 128)
    mst[:, 32:64] = total[:, 128:256].reshape(NX, 32, 128)
    x_copies = []
    for k, d in enumerate((2, 1, 3)):
        copy = push(mst.at[lax.rem(x + d, NX)], xr.at[k], xs.at[k], xrs.at[k], along_x(d))
        copy.start()
        x_copies.append(copy)
    loop(direct, w, lambda v: right_tile(v).start())
    for copy in p0_copies:
        copy.wait_recv()
    row = iota((128, 32), 0)
    source = (row >> 5) * 8 + ((row >> 2) & 3) * 2 + ((row >> 4) & 1)
    spread = jnp.where(iota((128, 32), 1) == source, 1.0, 0.0).astype(BF)
    tiles = p0x[...].astype(F32).reshape(32, 128).astype(BF)
    spread = mm(spread, tiles, ((1,), (0,)))
    mine = (iota((128, 128), 1) >> 5) == (iota((128, 128), 0) & 3)
    spread = jnp.where(mine, spread, 0.0).astype(BF)
    comb = jnp.where((iota((32, 128), 1) & 31) == iota((32, 128), 0), 1.0, 0.0).astype(BF)
    gst[...] = mm(comb, spread, ((1,), (1,))).reshape(32, 1, 128)

    @pl.when(w > 0)
    def _():
        p0g[w, 1] = gst[z]

    @pl.when(early)
    def _():
        left_rows_root(p0r.at[w]).start()

    @pl.when(w >= HALF)
    def _():
        left_rows_root(pr.at[1]).start()

    @pl.when(w == 0)
    def _():
        p0g[w] = gst[0:3]

    loop(1, w, lambda v: left_row(v).start())

    for copy in x_copies:
        copy.wait_recv()
    value = mst[x] + xr[0] + xr[1] + xr[2]
    s1[...] = value

    def parent_of(v):
        parent = 0
        for hub, first, stop in HUBS:
            parent = jnp.where((v >= first) & (v < stop), hub, parent)
        return parent

    def to_parent():
        return push(s1b, mr.at[w], ms.at[NZ], mrs.at[w], along_z(parent_of(w)))

    def add(v):
        push(s1b, mr.at[v], ms.at[NZ], mrs.at[v], along_z(v)).wait_recv()
        s1[...] += mr[v].astype(F32)

    for hub, first, stop in HUBS:

        @pl.when(w == hub)
        def _():
            loop(first, stop, add)

        if hub > first:

            @pl.when((w >= first) & (w < stop))
            def _():
                pl.semaphore_wait(ready, 1)

    s1b[...] = s1[...].astype(WIRE)

    @pl.when(w > 0)
    def _():
        to_parent().start()

    def add_direct(v):
        @pl.when(parent_of(v) == 0)
        def _():
            add(v)

    def late_to(v):
        tiles = p1g.at[pl.ds(HALF, NZ - HALF)]
        return push(tiles, tiles, ls.at[v], lr, along_z(v))

    def answer(v):
        right_tile(v).start()
        left_row(v).start()

    def landed_tile(v):
        push(p1g.at[v], p1g.at[v], p1s.at[v], p1r.at[v], along_z(v)).wait_recv()

    def landed(v):

        @pl.when((v < HALF) | (w >= HALF))
        def _():
            landed_tile(v)

        push(
            gst.at[pl.ds(0, 1)], p0g.at[v, pl.ds(1, 1)], p0s.at[v], p0r.at[v], along_z(v)
        ).wait_recv()

    def landed_root(v):
        landed_tile(v)
        push(gst.at[pl.ds(0, 3)], p0g.at[v], p0s.at[v], p0r.at[v], along_z(v)).wait_recv()

    @pl.when(w == 0)
    def _():
        def meet(v):
            landed_root(v)
            answer(v)

            @pl.when(v > LAG)
            def _():
                add_direct(v - LAG)

        loop(1, HALF, meet)
        tiles = p1g.at[pl.ds(HALF, NZ - HALF)]
        push(tiles, tiles, p1s.at[0], pr.at[0], along_z(1)).wait_recv()
        for v in ROOT_UP:
            late_to(v).start()
        some = p0g.at[pl.ds(HALF, NZ - HALF)]
        push(some, some, p0s.at[0], pr.at[1], along_z(1)).wait_recv()

    @pl.when((w > 0) & (w < last))
    def _():
        def meet(v):
            landed(v)
            answer(v)

        loop(w + 1, last, meet)
        landed(last)
        loop(0, w, landed)

    def prepare(slot):
        rows_ = p0g[:, slot].reshape(32, 128).astype(BF)
        places = lax.rem(iota((32, 128), 0) + 1, NZ)
        placed = jnp.where((iota((32, 128), 1) & 31) == places, 1.0, 0.0).astype(BF)
        gathered = mm(rows_, placed, ((0,), (0,)))
        mine_ = (iota((128, 128), 1) >> 5) == (iota((128, 128), 0) >> 5)
        lft[slot] = jnp.where(mine_, gathered, 0.0).reshape(4, 32, 128).sum(axis=0).astype(BF)

    def project(slot):
        left = lft[slot]
        halves = []
        for part in (0, 1):
            high, low = split(tm[32 * part : 32 * part + 32])
            halves.append(mm(left, high, ((1,), (1,))) + mm(left, low, ((1,), (1,))))
        with_real, with_imag = halves
        x_real = with_real[0:16] + with_imag[16:32]
        x_imag = with_imag[0:16] - with_real[16:32]
        high, low = split(jnp.concatenate([x_real, x_imag], axis=0))
        stacked = jnp.concatenate([high, low], axis=0)
        for spin in range(4):
            made = []
            for part in (0, 1):
                right = p1f[pl.ds(2 * spin + part, NZ, stride=8), :].astype(BF)
                full = mm(stacked, right, ((1,), (0,)))
                made.append(full[0:32] + full[32:64])
            ast[spin, 0] = made[0][0:16] - made[1][16:32]
            ast[spin, 1] = made[1][0:16] + made[0][16:32]
        for gamma in range(count):
            real = imag = None
            for spin in range(4):
                col = columns[spin, gamma]
                power = phases[spin, gamma]
                cr = jnp.where(power == 0, factor, 0.0) - jnp.where(power == 2, factor, 0.0)
                ci = jnp.where(power == 1, factor, 0.0) - jnp.where(power == 3, factor, 0.0)
                a_real = ast[col, 0, 4 * spin : 4 * spin + 4, :]
                a_imag = ast[col, 1, 4 * spin : 4 * spin + 4, :]
                part_r = cr * a_real - ci * a_imag
                part_i = cr * a_imag + ci * a_real
                real = part_r if real is None else real + part_r
                imag = part_i if imag is None else imag + part_i
            for k in range(NX):
                ost[slot, k, 2 * gamma : 2 * gamma + 1, :] = real[k : k + 1]
                ost[slot, k, 2 * gamma + 1 : 2 * gamma + 2, :] = imag[k : k + 1]

    def total_to(v):
        return push(tm, tm, ms.at[v], tr, along_z(v))

    upward = w < HALF

    def relay_up(act):
        @pl.when(upward & (w > 0) & (lax.rem(w, STEP) == 0))
        def _():
            far = jnp.minimum(w + STEP, HALF - 1)
            loop(0, far - w, lambda i: act(far - i))

    def relay(act):
        relay_up(act)
        for hub_w, first, stop in DOWN:

            @pl.when(w == hub_w)
            def _():
                loop(first, stop, act)

    def spread_tiles():
        flat = p1g[...].astype(F32).reshape(NZ * 8, 128)
        p1f[8 : NZ * 8] = flat[0 : NZ * 8 - 8]
        p1f[0:8] = flat[NZ * 8 - 8 :]

    def relay_root(act):
        for v in ROOT_UP + ROOT_DOWN:
            act(v)

    def rows_to_last(k):
        return push(
            ost.at[0, k], orv.at[x], o0s.at[k], ors.at[x], {"space_0": k, "space_1": zof(last)}
        )

    def rows_to_next(k):
        return push(
            ost.at[2, k], orv.at[x], o2s.at[k], ors.at[x], {"space_0": k, "space_1": zof(1)}
        )

    def rows_to_x(d):
        k = lax.rem(x + d, NX)
        return push(ost.at[1, k], orv.at[x], os_.at[d - 1], ors.at[x], along_x(d))

    def rows_from(k):
        push(ost.at[1, k], orv.at[k], os_.at[0], ors.at[k], along_x(1)).wait_recv()

    @pl.when(w == 0)
    def _():
        prepare(0)
        spread_tiles()

        loop(HALF - LAG, HALF, add_direct)
        loop(HALF, last, answer)
        loop(HALF, NZ, add_direct)
        tm[...] = s1[...]
        for v in ROOT_UP:
            total_to(v).start()
        project(0)
        for d in (2, 1, 3, 0):
            rows_to_last(lax.rem(x + d, NX)).start()
        prepare(1)
        prepare(2)
        for v in ROOT_DOWN:
            total_to(v).start()

    @pl.when((w > 1) & (w < last))
    def _():
        prepare(1)

    @pl.when((w > 1) & upward)
    def _():
        late_to(w).wait_recv()

    relay_up(lambda v: late_to(v).start())

    @pl.when((w > 1) & (w < last))
    def _():
        total_to(w).wait_recv()

    relay(lambda v: total_to(v).start())

    @pl.when((w > 1) & (w < last))
    def _():
        spread_tiles()

    own = (w < last) & (w != 1)

    @pl.when(own)
    def _():
        project(1)
        for d in (2, 1, 3):
            rows_to_x(d).start()

    @pl.when(w == 0)
    def _():
        project(2)
        for k in range(NX):
            rows_to_next(k).start()

    for copy in x_copies + p0_copies:
        copy.wait_send()

    @pl.when(w > 0)
    def _():
        to_parent().wait_send()
        left_rows_root(pr.at[1]).wait_send()

    @pl.when(w > 0)
    def _():
        tile_root(pr.at[0]).wait_send()

    loop(direct, w, lambda v: right_tile(v).wait_send())
    loop(1, w, lambda v: left_row(v).wait_send())

    def answered(v):
        right_tile(v).wait_send()
        left_row(v).wait_send()

    loop(w + 1, last, answered)

    @pl.when(own)
    def _():
        for d in (1, 3, 2):
            rows_from(lax.rem(x + d, NX))
        orv[x] = ost[1, x]

    @pl.when(~own)
    def _():
        for k in range(NX):
            rows_from(k)

    out[...] = orv[0] + orv[1] + orv[2] + orv[3]

    @pl.when(w == 0)
    def _():
        relay_root(lambda v: total_to(v).wait_send())
        for v in ROOT_UP:
            late_to(v).wait_send()

        for k in range(NX):
            rows_to_last(k).wait_send()
            rows_to_next(k).wait_send()

    relay(lambda v: total_to(v).wait_send())
    relay_up(lambda v: late_to(v).wait_send())

    @pl.when(own)
    def _():
        for d in (2, 1, 3):
            rows_to_x(d).wait_send()


def on_device(eigvecs, perambulator, momenta, source_slots, gamma_columns, gamma_phases):
    local_sites = eigvecs.shape[1]
    eig_count = eigvecs.shape[4]
    store_count = perambulator.shape[1]
    total_sites = local_sites * lax.axis_size(SPACE)
    extent_x = total_sites // (LY * LZ)
    lines = local_sites // LZ
    rows = LZ * 6
    assert local_sites == lines * LZ and eig_count == NX * NZ == 128 and lines <= 8
    count = gamma_columns.shape[0]
    vmem = lambda shape, dtype=F32: pltpu.VMEM(shape, dtype)
    dma = lambda n: pltpu.SemaphoreType.DMA((n,))

    meson = pl.pallas_call(
        functools.partial(
            kernel, lines, rows, extent_x, 1.0 / math.sqrt(12.0 * total_sites), count
        ),
        out_shape=pltpu.VMEM((2 * count, 128), F32),
        in_specs=[pl.BlockSpec(memory_space=pltpu.HBM)] * 6,
        out_specs=pl.BlockSpec(memory_space=pltpu.VMEM),
        scratch_shapes=[
            pltpu.SMEM(momenta.shape, jnp.int32),
            pltpu.SMEM(source_slots.shape, jnp.int32),
            pltpu.SMEM(gamma_columns.shape[::-1], jnp.int32),
            pltpu.SMEM(gamma_phases.shape[::-1], jnp.int32),
            vmem((lines * rows, 128), BF),
            vmem((store_count, 8, 128), BF),
            vmem((rows, 128)),
            vmem((rows, 128)),
            vmem((8, 128)),
            vmem((8, 128)),
            vmem((NX, 64, 128)),
            vmem((3, 64, 128)),
            vmem((64, 128)),
            vmem((64, 128), WIRE),
            vmem((NZ, 64, 128), WIRE),
            vmem((64, 128)),
            vmem((NX, 8, 128), BF),
            vmem((NZ, 1, 128)),
            vmem((NZ, 3, 1, 128)),
            vmem((NZ, 8, 128), BF),
            vmem((NZ * 8, 128)),
            vmem((3, 32, 128), BF),
            vmem((4, 2, 16, 128)),
            vmem((3, NX, 2 * count, 128)),
            vmem((NX, 2 * count, 128)),
            dma(6),
            pltpu.SemaphoreType.REGULAR,
            dma(2),
            dma(3), dma(3), dma(3), dma(3),
            dma(NZ), dma(NZ), dma(NZ), dma(NZ), dma(NZ + 1), dma(NZ),
            pltpu.SemaphoreType.DMA,
            dma(NZ), pltpu.SemaphoreType.DMA,
            dma(3), dma(NX), dma(NX), dma(NX),
        ],
        compiler_params=pltpu.CompilerParams(
            collective_id=0, has_side_effects=True, vmem_limit_bytes=63043328
        ),
        name="meson",
    )(
        eigvecs.reshape(local_sites * 6, eig_count),
        perambulator.reshape(store_count, 8, eig_count),
        momenta,
        source_slots,
        gamma_columns.T,
        gamma_phases.T,
    )
    return meson.reshape(1, 1, 1, count, 2, eig_count)


def solution(mesh):
    split_mesh = Mesh(
        mesh.devices.reshape(mesh.shape["cfg"], NX, NZ, mesh.shape["tm"]),
        ("cfg", "space_0", "space_1", "tm"),
    )
    placed = (
        P(("cfg", "tm"), SPACE, None, None, None),
        P(("cfg", "tm"), None, None, None, SPACE, None),
        P(),
        P(),
        P(),
        P(),
    )
    return jax.shard_map(
        on_device,
        mesh=split_mesh,
        in_specs=placed,
        out_specs=P(("cfg", "tm"), SPACE, None, None, None, None),
        check_vma=False,
    )
```
